128 devices in a mesh: blk: 32 (over x, z, core), grp: 4 (over y).
Axes of the slice: x: 4, y: 4, z: 4, core: 2. Of those that a mesh axis runs over, the one named last changes fastest.
Arguments:
- statistics: float32 [4, 64, 512, 512], P('grp', 'blk'), as said below
- gradients: bfloat16 [4, 16, 512, 14336], P('grp', None, None, 'blk'), may hold values from -6 to 6
- live_counts: int32 [4, 32], P('grp'), may hold values from 0 to 2, as said below
- slot_row: int32 [4, 64], P('grp'), may hold values from 0 to 15, as said below
- sweeps: int32 [4, 64], P('grp', 'blk'), may hold values from 1 to 2, as said below
Outputs:
- updates: bfloat16 [4, 16, 512, 14336], P('grp', None, None, 'blk')
- off_max: float32 [2], replicated
The draws below stay inside these ranges and needn't reach their ends.
Inputs may be any that keep to these rules, and one draw needn't show every extreme that they name: `live_counts`: the live slots of one index of grp number exactly 16; in every draw some device of each grp index has 2 live slots. `slot_row`: over the live slots of one index of grp each row block 0 to 15 appears exactly once. In each index of grp some live slot has 2 sweeps. `statistics`: every block is symmetric positive definite.
All inputs are finite; a program needn't handle non-finite values.
Results may differ from the reference program's by a relative error of at most 0.0051.
Values may be sent and summed in bfloat16 or wider, within the bound.
A program may use at most 192 MiB of HBM per device.

```python
import jax
import jax.numpy as jnp
from jax import lax

FF = 14336
BLOCK = 512
SLOTS = 2
ROWB = 16
MAXS = 2
N_BLK = 32
N_GRP = 4


def layout(base_key):
    slot_total = N_BLK * SLOTS

    def one_group(row_key):
        keys_list = jax.random.split(row_key, 5)
        heavy_owner = jax.random.randint(keys_list[0], (), 0, N_BLK)
        partner_owner = (heavy_owner + N_BLK // 2) % N_BLK
        priority = jax.random.permutation(keys_list[1], slot_total).astype(jnp.int32)
        slot_ids = lax.iota(jnp.int32, slot_total)
        owner_of = slot_ids // SLOTS
        local_slot = slot_ids % SLOTS
        priority = jnp.where(owner_of == heavy_owner, local_slot - SLOTS, priority)
        priority = jnp.where(owner_of == partner_owner, slot_total + local_slot, priority)
        ranking = jnp.argsort(priority, stable=True)
        picked = jnp.zeros((slot_total,), jnp.int32).at[ranking[:ROWB]].set(1)
        counts = jnp.sum(picked.reshape(N_BLK, SLOTS), axis=1).astype(jnp.int32)
        offsets = jnp.cumsum(counts) - counts
        live_slot = local_slot < counts[owner_of]
        row_order = jax.random.permutation(keys_list[2], ROWB).astype(jnp.int32)
        position = jnp.clip(offsets[owner_of] + local_slot, 0, ROWB - 1)
        filler = jax.random.randint(keys_list[3], (slot_total,), 0, ROWB)
        rows_drawn = jnp.where(live_slot, row_order[position], filler).astype(jnp.int32)
        sweep_drawn = jax.random.randint(keys_list[4], (slot_total,), 1, MAXS + 1)
        sweep_drawn = jnp.where(slot_ids == heavy_owner * SLOTS, MAXS, sweep_drawn).astype(jnp.int32)
        return (counts, rows_drawn, sweep_drawn)
    return jax.vmap(one_group)(jax.random.split(jax.random.fold_in(base_key, 11), N_GRP))


def draw_live_counts(key, part):
    return layout(key)[0]


def draw_slot_row(key, part):
    return layout(key)[1]


def draw_sweeps(key, part):
    return layout(key)[2]


def draw_statistics(key, part):
    slot_total = N_BLK * SLOTS
    samples = 2 * BLOCK
    item_keys = jax.random.split(jax.random.fold_in(key, 5), N_GRP * slot_total)

    def one_block(item_key):
        keys_list = jax.random.split(item_key, 2)
        noise = jax.random.normal(keys_list[0], (BLOCK, samples), jnp.float32)
        scales = jnp.exp(jax.random.uniform(keys_list[1], (BLOCK,), jnp.float32, 0.0, jnp.log(10.0)))
        product = jnp.dot(noise, noise.T, precision=lax.Precision.HIGHEST) / samples
        product = 0.5 * (product + product.T)
        return scales[:, None] * product * scales[None, :] + 0.05 * jnp.eye(BLOCK, dtype=jnp.float32)
    blocks_all = lax.map(one_block, item_keys)
    return blocks_all.reshape(N_GRP, slot_total, BLOCK, BLOCK)


def shard_levels(own_key, shape, shards, least, high):
    gain = 1.0
    for axis_at, shards_of in shards:
        steps = jax.random.uniform(jax.random.fold_in(jax.random.fold_in(own_key, 6), axis_at), (shards_of,), jnp.float32, least / len(shards), high / len(shards))
        gain = gain * jnp.repeat(jnp.exp(steps), shape[axis_at] // shards_of).reshape((-1,) + (1,) * (len(shape) - 1 - axis_at))
    return gain


def scatter_about(key, shape, spread, bound, cuts=(), kind=jnp.bfloat16):
    factor_of = shard_levels(key, shape, cuts, -0.22, 0.18) if cuts else 1.0
    drawn = jax.random.normal(key, shape, jnp.float32) * spread * factor_of
    return jnp.minimum(jnp.maximum(drawn, -bound), bound).astype(kind)


def setup_inputs(seed: int = 0) -> dict:
    arg_keys = jax.random.split(jax.random.key(seed), 6)
    statistics = draw_statistics(jax.random.fold_in(arg_keys[5], 71), 0)
    gradients = scatter_about(arg_keys[1], (N_GRP, ROWB, BLOCK, FF), 1.0, 6.0, ((0, 4), (3, 32)))
    live_counts = draw_live_counts(jax.random.fold_in(arg_keys[5], 71), 0)
    slot_row = draw_slot_row(jax.random.fold_in(arg_keys[5], 71), 0)
    sweeps = draw_sweeps(jax.random.fold_in(arg_keys[5], 71), 0)
    return dict(statistics=statistics, gradients=gradients, live_counts=live_counts, slot_row=slot_row, sweeps=sweeps)


damping = 0.01
pairings = ((0, 1, 2, 3), (0, 2, 1, 3), (0, 3, 1, 2))
highest = lax.Precision.HIGHEST

def regroup_cols(values, pairing, group_width):
    return jnp.concatenate([values[:, member * group_width:(member + 1) * group_width] for member in pairing], axis=1)

def regroup(values, pairing, group_width):
    stacked = jnp.concatenate([values[member * group_width:(member + 1) * group_width] for member in pairing], axis=0)
    return regroup_cols(stacked, pairing, group_width)

def generator(square_sub):
    group_width = square_sub.shape[-1] // 2
    diagonal = jnp.diagonal(square_sub, axis1=1, axis2=2)
    lower_diag = diagonal[:, :group_width, None]
    upper_diag = diagonal[:, None, group_width:]
    coupling = square_sub[:, :group_width, group_width:]
    difference = upper_diag - lower_diag
    bottom = difference * difference + 4.0 * coupling * coupling + damping * (lower_diag + upper_diag) ** 2
    angles = coupling * difference / bottom
    blank = jnp.zeros_like(angles)
    top_half = jnp.concatenate([blank, angles], axis=2)
    low_half = jnp.concatenate([-jnp.swapaxes(angles, 1, 2), blank], axis=2)
    return jnp.concatenate([top_half, low_half], axis=1)

def cayley(skew_part):
    order_size = skew_part.shape[-1]
    identity = jnp.eye(order_size, dtype=jnp.float32)
    square = jnp.einsum('hij,hjk->hik', skew_part, skew_part, precision=highest)
    numerator = identity + skew_part + 0.25 * square
    denominator = identity - 0.25 * square
    factor = jnp.linalg.cholesky(denominator)
    return jax.scipy.linalg.cho_solve((factor, True), numerator)

def rotate_round(matrix, vectors, pairing):
    block_size = matrix.shape[0]
    group_width = block_size // 4
    restore = [pairing.index(member) for member in range(4)]
    matrix = regroup(matrix, pairing, group_width)
    vectors = regroup_cols(vectors, pairing, group_width)
    half_size = 2 * group_width
    square_sub = jnp.stack([matrix[:half_size, :half_size], matrix[half_size:, half_size:]])
    rotation = cayley(generator(square_sub))
    row_part = jnp.einsum('hpq,hpc->hqc', rotation, matrix.reshape(2, half_size, block_size), precision=highest)
    row_part = row_part.reshape(block_size, block_size)
    matrix = jnp.einsum('rhp,hpq->rhq', row_part.reshape(block_size, 2, half_size), rotation, precision=highest)
    matrix = matrix.reshape(block_size, block_size)
    vectors = jnp.einsum('rhp,hpq->rhq', vectors.reshape(block_size, 2, half_size), rotation, precision=highest)
    vectors = vectors.reshape(block_size, block_size)
    return (regroup(matrix, restore, group_width), regroup_cols(vectors, restore, group_width))

def one_sweep(matrix, vectors):
    for pairing in pairings:
        matrix, vectors = rotate_round(matrix, vectors, pairing)
    return (matrix, vectors)

def off_norm(matrix):
    block_size = matrix.shape[0]
    on_diagonal = lax.broadcasted_iota(jnp.int32, (block_size, block_size), 0) == lax.broadcasted_iota(jnp.int32, (block_size, block_size), 1)
    outside = jnp.where(on_diagonal, 0.0, matrix)
    return jnp.sqrt(jnp.sum(outside * outside) / jnp.sum(matrix * matrix))

def root_factor(matrix, vectors):
    scales = jnp.power(jnp.diagonal(matrix), -0.25)
    return jnp.dot(vectors * scales[None, :], vectors.T, precision=highest).astype(jnp.bfloat16)

def pick(group_stats, group_slots):
    return jnp.take(group_stats, group_slots, axis=0)

def reference(statistics, gradients, live_counts, slot_row, sweeps):
    slot_total = N_BLK * SLOTS
    slot_ids = lax.iota(jnp.int32, slot_total)
    row_ids = lax.iota(jnp.int32, ROWB)
    is_live = slot_ids[None, :] % SLOTS < jnp.repeat(live_counts, SLOTS, axis=1)
    matches = (slot_row[:, None, :] == row_ids[None, :, None]) & is_live[:, None, :]
    slot_of = lax.optimization_barrier(jnp.sum(jnp.where(matches, slot_ids[None, None, :], 0), axis=2)).astype(jnp.int32)
    chosen = jax.vmap(pick)(statistics, slot_of)
    chosen_sweeps = jax.vmap(pick)(sweeps, slot_of)
    blocks_flat = chosen.reshape(N_GRP * ROWB, BLOCK, BLOCK)
    sweeps_flat = chosen_sweeps.reshape(N_GRP * ROWB)
    identity = jnp.eye(BLOCK, dtype=jnp.float32)

    def process(payload):
        matrix, sweep_count = payload
        vectors = identity
        off_norms = []
        for sweep_index in range(MAXS):
            new_matrix, new_vectors = one_sweep(matrix, vectors)
            active = sweep_count > sweep_index
            matrix = jnp.where(active, new_matrix, matrix)
            vectors = jnp.where(active, new_vectors, vectors)
            off_norms.append(jnp.where(active, off_norm(new_matrix), jnp.float32(0.0)))
        return (root_factor(matrix, vectors), jnp.stack(off_norms))
    factors, all_norms = lax.map(process, (blocks_flat, sweeps_flat))
    off_max = lax.optimization_barrier(jnp.max(all_norms, axis=0))

    def apply_one(payload):
        factor, gradient = payload
        product = jnp.dot(factor.astype(jnp.float32), gradient.astype(jnp.float32), precision=highest)
        return product.astype(jnp.bfloat16)
    grads_flat = gradients.reshape(N_GRP * ROWB, BLOCK, FF)
    updates = lax.map(apply_one, (factors, grads_flat)).reshape(N_GRP, ROWB, BLOCK, FF)
    return (updates, off_max)
```

```python
import functools

import jax
import jax.numpy as jnp
from jax import lax
from jax.experimental import pallas as pl
from jax.experimental.pallas import tpu as pltpu
from jax.sharding import PartitionSpec as P

MAXS = 2

damping = 0.01
pairings = ((0, 1, 2, 3), (0, 2, 1, 3), (0, 3, 1, 2))
kappa_steps = (1.16, 1.74, 3.17, 6.2, 12.3, 24.5, 49.0, 98.0, 196.0)
bf16 = jnp.bfloat16
f32 = jnp.float32


def split(values):
    high = values.astype(bf16)
    return high, (values - high.astype(f32)).astype(bf16)


def left_parts(parts):
    high, low = parts
    return jnp.concatenate([high, high, low], axis=1)


def right_parts(parts):
    high, low = parts
    return jnp.concatenate([high, low, high], axis=0)


def dot(left, right):
    return jnp.dot(left, right, preferred_element_type=f32)


def dot3(left, right):
    return dot(left_parts(split(left)), right_parts(split(right)))


def eye_mask(size):
    shape = (size, size)
    return lax.broadcasted_iota(jnp.int32, shape, 0) == lax.broadcasted_iota(jnp.int32, shape, 1)


def angles_of(lower, coupling, upper, on_diagonal):
    lower_diag = jnp.sum(jnp.where(on_diagonal, lower, 0.0), axis=1, keepdims=True)
    upper_diag = jnp.sum(jnp.where(on_diagonal, upper, 0.0), axis=0, keepdims=True)
    difference = upper_diag - lower_diag
    total = lower_diag + upper_diag
    bottom = difference * difference + 4.0 * coupling * coupling + damping * (total * total)
    return coupling * difference / bottom


def jacobi_kernel(
    stats_ref, counts_ref, sweeps_ref, packed_ref, off_ref,
    mat, vec_high, vec_low, mid_high, mid_low, angle, powers,
):
    slot_count, size, _ = mat.shape
    width = size // 4
    rank = lax.axis_index("blk")
    own_live = counts_ref[0, rank]
    on_diagonal = eye_mask(width)
    identity = jnp.where(on_diagonal, 1.0, 0.0).astype(f32)

    def span(member):
        return pl.ds(member * width, width)

    def one_round(slots, pairing):
        pairs = (pairing[:2], pairing[2:])
        chains = [(at, slot, half) for at, slot in enumerate(slots) for half in range(2)]
        outers = []
        peak = jnp.zeros((1, width), f32)
        for at, slot, half in chains:
            first, second = pairs[half]
            angles = angles_of(
                mat[slot, span(first), span(first)],
                mat[slot, span(first), span(second)],
                mat[slot, span(second), span(second)],
                on_diagonal,
            )
            angle[2 * at + half] = angles
            outer = dot3(angles, angles.T)
            outers.append(outer)
            peak = jnp.maximum(peak, jnp.sum(jnp.abs(outer), axis=0, keepdims=True))
        kappa = 1.0 + 0.26 * jnp.max(peak)
        count = jnp.int32(0)
        for bound in kappa_steps:
            count = count + (kappa > bound).astype(jnp.int32)
        scale = 2.0 / (1.0 + jnp.full((1, width), kappa))
        for at, slot, half in chains:
            error = (1.0 - scale) * identity - (0.25 * scale) * outers[2 * at + half]
            powers[2 * at + half, :, :width] = scale * (identity + error)
            powers[2 * at + half, :, width:] = dot3(error, error)

        def double(step, carry):
            for at, slot, half in chains:
                both = powers[2 * at + half]
                high, low = split(both)
                product = dot(
                    left_parts((high[:, width:], low[:, width:])), right_parts((high, low))
                )
                powers[2 * at + half, :, :width] = both[:, :width] + product[:, :width]
                powers[2 * at + half, :, width:] = product[:, width:]
            return carry

        lax.fori_loop(0, count, double, 0)

        flips = {}
        for at, slot, half in chains:
            first, second = pairs[half]
            angles = angle[2 * at + half]
            inverse = powers[2 * at + half, :, :width]
            inverse = inverse + dot(
                inverse.astype(bf16), powers[2 * at + half, :, width:].astype(bf16)
            )
            top_right = dot3(inverse, angles)
            flip_right = top_right.T
            low_right = identity - 0.5 * dot3(angles.T, top_right)
            top = split(2.0 * inverse - identity)
            right = split(top_right)
            flip = split(flip_right)
            low = split(low_right)

            def square(kind, flipped):
                above, below = (-right[kind], flip[kind]) if flipped else (right[kind], -flip[kind])
                return jnp.concatenate(
                    [
                        jnp.concatenate([top[kind], above], axis=1),
                        jnp.concatenate([below, low[kind]], axis=1),
                    ],
                    axis=0,
                )

            flips[at, half] = left_parts((square(0, True), square(1, True)))
            rotation = right_parts((square(0, False), square(1, False)))
            for members in (pairs[0],) if half == 0 else pairs:
                rows = jnp.concatenate(
                    [
                        jnp.concatenate(
                            [mat[slot, span(member), span(column)] for column in pairs[half]],
                            axis=1,
                        )
                        for member in members
                    ],
                    axis=0,
                )
                middle = split(dot(left_parts(split(rows)), rotation))
                for down, member in enumerate(members):
                    for across, column in enumerate(pairs[half]):
                        tall = slice(down * width, (down + 1) * width)
                        wide = slice(across * width, (across + 1) * width)
                        mid_high[slot, span(member), span(column)] = middle[0][tall, wide]
                        mid_low[slot, span(member), span(column)] = middle[1][tall, wide]
            columns = tuple(
                jnp.concatenate([ref[slot, :, span(first)], ref[slot, :, span(second)]], axis=1)
                for ref in (vec_high, vec_low)
            )
            turned = split(dot(left_parts(columns), rotation))
            for place, member in enumerate((first, second)):
                inner = slice(place * width, (place + 1) * width)
                vec_high[slot, :, span(member)] = turned[0][:, inner]
                vec_low[slot, :, span(member)] = turned[1][:, inner]
        for at, slot, half in chains:
            order = pairs[0] + pairs[1] if half == 0 else pairs[1]
            rows = tuple(
                jnp.concatenate(
                    [
                        jnp.concatenate(
                            [ref[slot, span(member), span(column)] for column in order], axis=1
                        )
                        for member in pairs[half]
                    ],
                    axis=0,
                )
                for ref in (mid_high, mid_low)
            )
            fresh = dot(flips[at, half], right_parts(rows))
            for down, member in enumerate(pairs[half]):
                for across, column in enumerate(order):
                    block = fresh[
                        down * width : (down + 1) * width, across * width : (across + 1) * width
                    ]
                    mat[slot, span(member), span(column)] = block
                    if across > 1:
                        mat[slot, span(column), span(member)] = block.T

    def measure(sweep, slot):
        outside = jnp.zeros((1, width), f32)
        inside = jnp.zeros((1, width), f32)
        for row in range(4):
            for column in range(4):
                squares = mat[slot, span(row), span(column)]
                squares = squares * squares
                if row == column:
                    own = jnp.where(on_diagonal, squares, 0.0)
                    inside += jnp.sum(own, axis=0, keepdims=True)
                    squares = jnp.where(on_diagonal, 0.0, squares)
                outside += jnp.sum(squares, axis=0, keepdims=True)
        off_total = jnp.sum(outside, axis=1, keepdims=True)
        total = off_total + jnp.sum(inside, axis=1, keepdims=True)
        norm = jnp.broadcast_to(jnp.sqrt(off_total / total), (1, width))
        row = pl.ds(sweep, 1)
        off_ref[row, :] = jnp.maximum(off_ref[row, :], norm)

    off_ref[...] = jnp.zeros_like(off_ref)
    packed_ref[...] = jnp.zeros_like(packed_ref)
    ident_rows = jnp.where(eye_mask(size), 1.0, 0.0).astype(bf16)

    for slot in range(slot_count):

        @pl.when(slot < own_live)
        def _():
            mat[slot] = stats_ref[0, slot]
            vec_high[slot] = ident_rows
            vec_low[slot] = jnp.zeros((size, size), bf16)

    def one_sweep(sweep, carry):
        active = [
            jnp.logical_and(slot < own_live, sweeps_ref[0, slot] > sweep)
            for slot in range(slot_count)
        ]

        def run(slots):
            for pairing in pairings:
                one_round(slots, pairing)
            for slot in slots:
                measure(sweep, slot)

        for slot in range(0, slot_count, 2):
            if slot + 1 == slot_count:
                pl.when(active[slot])(functools.partial(run, (slot,)))
                continue
            pl.when(jnp.logical_and(active[slot], active[slot + 1]))(
                functools.partial(run, (slot, slot + 1))
            )
            single = jnp.where(active[slot], slot, slot + 1)
            pl.when(jnp.logical_xor(active[slot], active[slot + 1]))(
                functools.partial(run, (single,))
            )
        return carry

    lax.fori_loop(0, MAXS, one_sweep, 0)

    for slot in range(slot_count):

        @pl.when(slot < own_live)
        def _():
            diagonal = jnp.concatenate(
                [
                    jnp.sum(
                        jnp.where(on_diagonal, mat[slot, span(member), span(member)], 0.0),
                        axis=0,
                        keepdims=True,
                    )
                    for member in range(4)
                ],
                axis=1,
            )
            scales = lax.rsqrt(jnp.sqrt(jnp.sqrt(diagonal)))
            vectors = vec_high[slot].astype(f32) + vec_low[slot].astype(f32)
            high, low = split(vectors * scales)
            left = jnp.concatenate([high, high, low], axis=1)
            right = jnp.concatenate([high, low, high], axis=1)
            start = 0
            for row in range(4):
                strip = lax.dot_general(
                    left[row * width : (row + 1) * width],
                    right[row * width :],
                    (((1,), (1,)), ((), ())),
                    preferred_element_type=f32,
                ).astype(bf16)
                for column in range(4 - row):
                    packed_ref[slot, start : start + width] = strip[
                        :, column * width : (column + 1) * width
                    ]
                    start += width


def jacobi(statistics, live_counts, sweeps, packed_rows):
    slot_count, size = statistics.shape[1], statistics.shape[2]
    width = size // 4
    vmem = pl.BlockSpec(memory_space=pltpu.VMEM)
    smem = pl.BlockSpec(memory_space=pltpu.SMEM)
    return pl.pallas_call(
        jacobi_kernel,
        name="jacobi",
        out_shape=(
            jax.ShapeDtypeStruct((slot_count, packed_rows, width), bf16),
            jax.ShapeDtypeStruct((8, width), f32),
        ),
        in_specs=[vmem, smem, smem],
        out_specs=(vmem, vmem),
        scratch_shapes=[
            pltpu.VMEM((slot_count, size, size), f32),
            pltpu.VMEM((slot_count, size, size), bf16),
            pltpu.VMEM((slot_count, size, size), bf16),
            pltpu.VMEM((slot_count, size, size), bf16),
            pltpu.VMEM((slot_count, size, size), bf16),
            pltpu.VMEM((4, width, width), f32),
            pltpu.VMEM((4, width, 2 * width), f32),
        ],
        compiler_params=pltpu.CompilerParams(vmem_limit_bytes=24 * 1024 * 1024),
        cost_estimate=pl.CostEstimate(
            flops=10**10, bytes_accessed=4 * slot_count * size * size, transcendentals=0
        ),
    )(statistics, live_counts, sweeps)


def far_first(count):
    return sorted(range(1, count), key=lambda step: abs(2 * step - count))


def exchange_kernel(
    peers, groups, packed_ref, peaks_ref, counts_ref, rows_ref, chosen_ref, off_ref,
    arrived, mine, gathered, peak_in, peak_own, peak_out,
    send_one, recv_one, send_two, recv_two, send_three, recv_three, send_peak, recv_peak, send_top, recv_top,
):
    rank = lax.axis_index("blk")
    group = lax.axis_index("grp")
    slot_count = packed_ref.shape[0]
    row_count, share = mine.shape[0], mine.shape[1]
    width = packed_ref.shape[2]
    inner, outer = gathered.shape[:2]
    partner = rank + (1 - 2 * lax.rem(rank, 2)) if inner == 2 else rank

    def remote(source, target, send_sem, recv_sem, axis, index):
        return pltpu.make_async_remote_copy(
            src_ref=source,
            dst_ref=target,
            send_sem=send_sem,
            recv_sem=recv_sem,
            device_id={axis: index},
            device_id_type=pl.DeviceIdType.MESH,
        )

    barrier = pltpu.get_barrier_semaphore()
    for step in range(1, peers):
        pl.semaphore_signal(
            barrier, inc=1, device_id={"blk": lax.rem(rank + step, peers)},
            device_id_type=pl.DeviceIdType.MESH,
        )
    for step in range(1, groups):
        pl.semaphore_signal(
            barrier, inc=1, device_id={"grp": lax.rem(group + step, groups)},
            device_id_type=pl.DeviceIdType.MESH,
        )
    pl.semaphore_wait(barrier, peers + groups - 2)

    firsts, peaks = [], []
    for step in range(1, peers):
        target = lax.rem(rank + step, peers)
        firsts.append(
            remote(
                packed_ref.at[:, pl.ds(pl.multiple_of(target * share, share), share)],
                arrived.at[step], send_one.at[step], recv_one.at[step], "blk", target,
            )
        )
        peaks.append(
            remote(
                peaks_ref, peak_in.at[step], send_peak.at[step], recv_peak.at[step], "blk", target
            )
        )
    for copy in peaks + [firsts[step - 1] for step in far_first(peers)]:
        copy.start()
    arrived[0] = packed_ref[:, pl.ds(pl.multiple_of(rank * share, share), share)]
    top = peaks_ref[...]
    for step, copy in enumerate(peaks, 1):
        copy.wait_recv()
        top = jnp.maximum(top, peak_in[step])
    peak_own[...] = top
    for copy in firsts:
        copy.wait_recv()
    for row in range(row_count):
        place = jnp.int32(0)
        for slot in range(peers * slot_count):
            owner, local = slot // slot_count, slot % slot_count
            match = jnp.logical_and(rows_ref[0, slot] == row, local < counts_ref[0, owner])
            spot = lax.rem(rank - owner + peers, peers) * slot_count + local
            place = jnp.where(match, spot, place)
        mine[row] = arrived[place // slot_count, lax.rem(place, slot_count)]
    seconds, tops = [], []
    for step in range(1, groups):
        tops.append(
            remote(
                peak_own, peak_out.at[step], send_top.at[step], recv_top.at[step],
                "grp", lax.rem(group + step, groups),
            )
        )
    for step in range(1, outer):
        seconds.append(
            remote(
                mine, gathered.at[0, step], send_two.at[step], recv_two.at[step],
                "blk", lax.rem(rank + step * inner, peers),
            )
        )
    thirds = []
    for step in range(outer if inner == 2 else 0):
        thirds.append(
            remote(
                gathered.at[0, step] if step else mine, gathered.at[1, step],
                send_three.at[step], recv_three.at[step], "blk", partner,
            )
        )
    for copy in tops + [seconds[step - 1] for step in far_first(outer)]:
        copy.start()
    if thirds:
        thirds[0].start()
    gathered[0, 0] = mine[...]
    for step in far_first(outer):
        seconds[step - 1].wait_recv()
        if thirds:
            thirds[step].start()
    for step, copy in enumerate(tops, 1):
        copy.wait_recv()
        top = jnp.maximum(top, peak_out[step])
    off_ref[...] = top
    for copy in thirds:
        copy.wait_recv()
    spots = []
    for owner in range(peers):
        side = lax.rem(rank + owner, inner)
        base = rank + side * (partner - rank)
        spots.append((side, lax.rem(base - owner + peers, peers) // inner))
    for row in range(row_count):
        whole = jnp.concatenate([gathered[side, spot, row] for side, spot in spots], axis=0)
        start = 0
        for above in range(4):
            for below in range(above, 4):
                block = whole[start : start + width]
                start += width
                first = slice(above * width, (above + 1) * width)
                second = slice(below * width, (below + 1) * width)
                chosen_ref[row, first, second] = block
                if above != below:
                    chosen_ref[row, second, first] = block.T
    for copy in firsts + peaks + tops + seconds + thirds:
        copy.wait_send()


def exchange(packed, peaks, live_counts, slot_row, row_count, size, peers, groups):
    slot_count, packed_rows, width = packed.shape
    share = packed_rows // peers
    inner = 1 if peers % 2 else 2
    outer = peers // inner
    vmem = pl.BlockSpec(memory_space=pltpu.VMEM)
    smem = pl.BlockSpec(memory_space=pltpu.SMEM)
    dma = pltpu.SemaphoreType.DMA
    return pl.pallas_call(
        functools.partial(exchange_kernel, peers, groups),
        name="exchange",
        out_shape=(
            jax.ShapeDtypeStruct((row_count, size, size), bf16),
            jax.ShapeDtypeStruct(peaks.shape, f32),
        ),
        in_specs=[vmem, vmem, smem, smem],
        out_specs=(vmem, vmem),
        scratch_shapes=[
            pltpu.VMEM((peers, slot_count, share, width), bf16),
            pltpu.VMEM((row_count, share, width), bf16),
            pltpu.VMEM((inner, outer, row_count, share, width), bf16),
            pltpu.VMEM((peers,) + peaks.shape, f32),
            pltpu.VMEM(peaks.shape, f32),
            pltpu.VMEM((groups,) + peaks.shape, f32),
            dma((peers,)), dma((peers,)), dma((outer,)), dma((outer,)), dma((outer,)),
            dma((outer,)), dma((peers,)), dma((peers,)), dma((groups,)), dma((groups,)),
        ],
        compiler_params=pltpu.CompilerParams(
            collective_id=0, has_side_effects=True, vmem_limit_bytes=16 * 1024 * 1024
        ),
        cost_estimate=pl.CostEstimate(
            flops=10**10, bytes_accessed=2 * row_count * size * size, transcendentals=0
        ),
    )(packed, peaks, live_counts, slot_row)


def update_kernel(chosen_ref, grads_ref, updates_ref):
    updates_ref[0, 0] = dot(grads_ref[0, 0], chosen_ref[0]).astype(bf16)


def update(chosen, gradients):
    row_count, columns, size = gradients.shape[1:]
    block = pl.BlockSpec((1, 1, columns, size), lambda row: (0, row, 0, 0))
    return pl.pallas_call(
        update_kernel,
        name="update",
        grid=(row_count,),
        out_shape=jax.ShapeDtypeStruct(gradients.shape, bf16),
        in_specs=[pl.BlockSpec((1, size, size), lambda row: (row, 0, 0)), block],
        out_specs=block,
        compiler_params=pltpu.CompilerParams(vmem_limit_bytes=16 * 1024 * 1024),
        cost_estimate=pl.CostEstimate(
            flops=2 * row_count * size * size * columns,
            bytes_accessed=2 * row_count * size * columns,
            transcendentals=0,
        ),
    )(chosen, gradients)


def per_device(peers, groups, statistics, gradients, live_counts, slot_row, sweeps):
    row_count, size = gradients.shape[1], gradients.shape[2]
    width = size // 4
    share = -(-10 * width // (16 * peers)) * 16
    packed, peaks = jacobi(statistics, live_counts, sweeps, share * peers)
    chosen, top = exchange(
        packed, peaks, live_counts, slot_row, row_count, size, peers, groups
    )
    updates = update(chosen, jnp.swapaxes(gradients, 2, 3))
    return (jnp.swapaxes(updates, 2, 3), top[:MAXS, 0])


def solution(mesh):
    in_specs = (
        P("grp", "blk", None, None),
        P("grp", None, None, "blk"),
        P("grp", None),
        P("grp", None),
        P("grp", "blk"),
    )
    out_specs = (P("grp", None, None, "blk"), P())
    return jax.shard_map(
        functools.partial(per_device, mesh.shape["blk"], mesh.shape["grp"]),
        mesh=mesh,
        in_specs=in_specs,
        out_specs=out_specs,
        check_vma=False,
    )
```

```python
import functools

import jax
import jax.numpy as jnp
from jax import lax
from jax.experimental import pallas as pl
from jax.experimental.pallas import tpu as pltpu
from jax.sharding import PartitionSpec as P

MAXS = 2

damping = 0.01
pairings = ((0, 1, 2, 3), (0, 2, 1, 3), (0, 3, 1, 2))
kappa_steps = (1.16, 1.74, 3.17, 6.2, 12.3, 24.5, 49.0, 98.0, 196.0)
bf16 = jnp.bfloat16
f32 = jnp.float32


def split(values):
    high = values.astype(bf16)
    return high, (values - high.astype(f32)).astype(bf16)


def left_parts(parts):
    high, low = parts
    return jnp.concatenate([high, high, low], axis=1)


def right_parts(parts):
    high, low = parts
    return jnp.concatenate([high, low, high], axis=0)


def dot(left, right):
    return jnp.dot(left, right, preferred_element_type=f32)


def dot3(left, right):
    return dot(left_parts(split(left)), right_parts(split(right)))


def eye_mask(size):
    shape = (size, size)
    return lax.broadcasted_iota(jnp.int32, shape, 0) == lax.broadcasted_iota(jnp.int32, shape, 1)


def angles_of(lower, coupling, upper, on_diagonal):
    lower_diag = jnp.sum(jnp.where(on_diagonal, lower, 0.0), axis=1, keepdims=True)
    upper_diag = jnp.sum(jnp.where(on_diagonal, upper, 0.0), axis=0, keepdims=True)
    difference = upper_diag - lower_diag
    total = lower_diag + upper_diag
    bottom = difference * difference + 4.0 * coupling * coupling + damping * (total * total)
    return coupling * difference / bottom


def jacobi_kernel(
    stats_ref, counts_ref, sweeps_ref, packed_ref, off_ref,
    mat, vec_high, vec_low, mid_high, mid_low, angle, powers,
):
    slot_count, size, _ = mat.shape
    width = size // 4
    rank = lax.axis_index("blk")
    own_live = counts_ref[0, rank]
    on_diagonal = eye_mask(width)
    identity = jnp.where(on_diagonal, 1.0, 0.0).astype(f32)

    def span(member):
        return pl.ds(member * width, width)

    def one_round(slots, pairing):
        pairs = (pairing[:2], pairing[2:])
        chains = [(at, slot, half) for at, slot in enumerate(slots) for half in range(2)]
        outers = []
        peak = jnp.zeros((1, width), f32)
        for at, slot, half in chains:
            first, second = pairs[half]
            angles = angles_of(
                mat[slot, span(first), span(first)],
                mat[slot, span(first), span(second)],
                mat[slot, span(second), span(second)],
                on_diagonal,
            )
            angle[2 * at + half] = angles
            outer = dot3(angles, angles.T)
            outers.append(outer)
            peak = jnp.maximum(peak, jnp.sum(jnp.abs(outer), axis=0, keepdims=True))
        kappa = 1.0 + 0.26 * jnp.max(peak)
        count = jnp.int32(0)
        for bound in kappa_steps:
            count = count + (kappa > bound).astype(jnp.int32)
        scale = 2.0 / (1.0 + jnp.full((1, width), kappa))
        for at, slot, half in chains:
            error = (1.0 - scale) * identity - (0.25 * scale) * outers[2 * at + half]
            powers[2 * at + half, :, :width] = scale * (identity + error)
            powers[2 * at + half, :, width:] = dot3(error, error)

        def double(step, carry):
            for at, slot, half in chains:
                both = powers[2 * at + half]
                high, low = split(both)
                product = dot(
                    left_parts((high[:, width:], low[:, width:])), right_parts((high, low))
                )
                powers[2 * at + half, :, :width] = both[:, :width] + product[:, :width]
                powers[2 * at + half, :, width:] = product[:, width:]
            return carry

        lax.fori_loop(0, count, double, 0)

        flips = {}
        for at, slot, half in chains:
            first, second = pairs[half]
            angles = angle[2 * at + half]
            inverse = powers[2 * at + half, :, :width]
            inverse = inverse + dot(
                inverse.astype(bf16), powers[2 * at + half, :, width:].astype(bf16)
            )
            top_right = dot3(inverse, angles)
            flip_right = top_right.T
            low_right = identity - 0.5 * dot3(angles.T, top_right)
            top = split(2.0 * inverse - identity)
            right = split(top_right)
            flip = split(flip_right)
            low = split(low_right)

            def square(kind, flipped):
                above, below = (-right[kind], flip[kind]) if flipped else (right[kind], -flip[kind])
                return jnp.concatenate(
                    [
                        jnp.concatenate([top[kind], above], axis=1),
                        jnp.concatenate([below, low[kind]], axis=1),
                    ],
                    axis=0,
                )

            flips[at, half] = left_parts((square(0, True), square(1, True)))
            rotation = right_parts((square(0, False), square(1, False)))
            for members in (pairs[0],) if half == 0 else pairs:
                rows = jnp.concatenate(
                    [
                        jnp.concatenate(
                            [mat[slot, span(member), span(column)] for column in pairs[half]],
                            axis=1,
                        )
                        for member in members
                    ],
                    axis=0,
                )
                middle = split(dot(left_parts(split(rows)), rotation))
                for down, member in enumerate(members):
                    for across, column in enumerate(pairs[half]):
                        tall = slice(down * width, (down + 1) * width)
                        wide = slice(across * width, (across + 1) * width)
                        mid_high[slot, span(member), span(column)] = middle[0][tall, wide]
                        mid_low[slot, span(member), span(column)] = middle[1][tall, wide]
            columns = tuple(
                jnp.concatenate([ref[slot, :, span(first)], ref[slot, :, span(second)]], axis=1)
                for ref in (vec_high, vec_low)
            )
            turned = split(dot(left_parts(columns), rotation))
            for place, member in enumerate((first, second)):
                inner = slice(place * width, (place + 1) * width)
                vec_high[slot, :, span(member)] = turned[0][:, inner]
                vec_low[slot, :, span(member)] = turned[1][:, inner]
        for at, slot, half in chains:
            order = pairs[0] + pairs[1] if half == 0 else pairs[1]
            rows = tuple(
                jnp.concatenate(
                    [
                        jnp.concatenate(
                            [ref[slot, span(member), span(column)] for column in order], axis=1
                        )
                        for member in pairs[half]
                    ],
                    axis=0,
                )
                for ref in (mid_high, mid_low)
            )
            fresh = dot(flips[at, half], right_parts(rows))
            for down, member in enumerate(pairs[half]):
                for across, column in enumerate(order):
                    block = fresh[
                        down * width : (down + 1) * width, across * width : (across + 1) * width
                    ]
                    mat[slot, span(member), span(column)] = block
                    if across > 1:
                        mat[slot, span(column), span(member)] = block.T

    def measure(sweep, slot):
        outside = jnp.zeros((1, width), f32)
        inside = jnp.zeros((1, width), f32)
        for row in range(4):
            for column in range(4):
                squares = mat[slot, span(row), span(column)]
                squares = squares * squares
                if row == column:
                    own = jnp.where(on_diagonal, squares, 0.0)
                    inside += jnp.sum(own, axis=0, keepdims=True)
                    squares = jnp.where(on_diagonal, 0.0, squares)
                outside += jnp.sum(squares, axis=0, keepdims=True)
        off_total = jnp.sum(outside, axis=1, keepdims=True)
        total = off_total + jnp.sum(inside, axis=1, keepdims=True)
        norm = jnp.broadcast_to(jnp.sqrt(off_total / total), (1, width))
        row = pl.ds(sweep, 1)
        off_ref[row, :] = jnp.maximum(off_ref[row, :], norm)

    off_ref[...] = jnp.zeros_like(off_ref)
    ident_rows = jnp.where(eye_mask(size), 1.0, 0.0).astype(bf16)

    for slot in range(slot_count):

        @pl.when(slot < own_live)
        def _():
            mat[slot] = stats_ref[0, slot]
            vec_high[slot] = ident_rows
            vec_low[slot] = jnp.zeros((size, size), bf16)

    def one_sweep(sweep, carry):
        active = [
            jnp.logical_and(slot < own_live, sweeps_ref[0, slot] > sweep)
            for slot in range(slot_count)
        ]

        def run(slots):
            for pairing in pairings:
                one_round(slots, pairing)
            for slot in slots:
                measure(sweep, slot)

        for slot in range(0, slot_count, 2):
            if slot + 1 == slot_count:
                pl.when(active[slot])(functools.partial(run, (slot,)))
                continue
            pl.when(jnp.logical_and(active[slot], active[slot + 1]))(
                functools.partial(run, (slot, slot + 1))
            )
            single = jnp.where(active[slot], slot, slot + 1)
            pl.when(jnp.logical_xor(active[slot], active[slot + 1]))(
                functools.partial(run, (single,))
            )
        return carry

    lax.fori_loop(0, MAXS, one_sweep, 0)

    for slot in range(slot_count):

        @pl.when(slot < own_live)
        def _():
            diagonal = jnp.concatenate(
                [
                    jnp.sum(
                        jnp.where(on_diagonal, mat[slot, span(member), span(member)], 0.0),
                        axis=0,
                        keepdims=True,
                    )
                    for member in range(4)
                ],
                axis=1,
            )
            scales = lax.rsqrt(jnp.sqrt(jnp.sqrt(diagonal)))
            vectors = vec_high[slot].astype(f32) + vec_low[slot].astype(f32)
            high, low = split(vectors * scales)
            left = jnp.concatenate([high, high, low], axis=1)
            right = jnp.concatenate([high, low, high], axis=1)
            start = 0
            for row in range(4):
                strip = lax.dot_general(
                    left[row * width : (row + 1) * width],
                    right[row * width :],
                    (((1,), (1,)), ((), ())),
                    preferred_element_type=f32,
                ).astype(bf16)
                for column in range(4 - row):
                    packed_ref[slot, start : start + width] = strip[
                        :, column * width : (column + 1) * width
                    ]
                    start += width


def jacobi(statistics, live_counts, sweeps, packed_rows):
    slot_count, size = statistics.shape[1], statistics.shape[2]
    width = size // 4
    vmem = pl.BlockSpec(memory_space=pltpu.VMEM)
    smem = pl.BlockSpec(memory_space=pltpu.SMEM)
    return pl.pallas_call(
        jacobi_kernel,
        name="jacobi",
        out_shape=(
            jax.ShapeDtypeStruct((slot_count, packed_rows, width), bf16),
            jax.ShapeDtypeStruct((MAXS, width), f32),
        ),
        in_specs=[vmem, smem, smem],
        out_specs=(vmem, vmem),
        scratch_shapes=[
            pltpu.VMEM((slot_count, size, size), f32),
            pltpu.VMEM((slot_count, size, size), bf16),
            pltpu.VMEM((slot_count, size, size), bf16),
            pltpu.VMEM((slot_count, size, size), bf16),
            pltpu.VMEM((slot_count, size, size), bf16),
            pltpu.VMEM((4, width, width), f32),
            pltpu.VMEM((4, width, 2 * width), f32),
        ],
        compiler_params=pltpu.CompilerParams(vmem_limit_bytes=24 * 1024 * 1024),
        cost_estimate=pl.CostEstimate(
            flops=10**10, bytes_accessed=4 * slot_count * size * size, transcendentals=0
        ),
    )(statistics, live_counts, sweeps)


def exchange_kernel(
    side, groups, packed_ref, peaks_ref, counts_ref, rows_ref, whole_ref, off_ref,
    arrived, mine, peak_in, peak_own, peak_out,
    send_one, recv_one, send_two, recv_two, send_near, recv_near, send_peak, recv_peak, send_top, recv_top,
):
    chips = side * side
    peers = 2 * chips
    rank = lax.axis_index("blk")
    group = lax.axis_index("grp")
    slot_count = packed_ref.shape[0]
    row_count, share = mine.shape[0], mine.shape[1]
    core = lax.rem(rank, 2)
    place_x, place_z = rank // (2 * side), lax.rem(rank // 2, side)
    partner = rank + 1 - 2 * core

    def remote(source, target, send_sem, recv_sem, axis, index):
        return pltpu.make_async_remote_copy(
            src_ref=source,
            dst_ref=target,
            send_sem=send_sem,
            recv_sem=recv_sem,
            device_id={axis: index},
            device_id_type=pl.DeviceIdType.MESH,
        )

    barrier = pltpu.get_barrier_semaphore()
    for step in range(1, peers):
        pl.semaphore_signal(
            barrier, inc=1, device_id={"blk": lax.rem(rank + step, peers)},
            device_id_type=pl.DeviceIdType.MESH,
        )
    for step in range(1, groups):
        pl.semaphore_signal(
            barrier, inc=1, device_id={"grp": lax.rem(group + step, groups)},
            device_id_type=pl.DeviceIdType.MESH,
        )
    pl.semaphore_wait(barrier, peers + groups - 2)

    def strip(index):
        return pl.ds(pl.multiple_of(index * share, share), share)

    firsts, peaks = [], []
    own_slots = pl.ds(rank * slot_count, slot_count)
    for step in range(1, peers):
        target = lax.rem(rank + step, peers)
        firsts.append(
            remote(
                packed_ref.at[:, strip(target)],
                arrived.at[own_slots], send_one.at[step], recv_one.at[step], "blk", target,
            )
        )
        peaks.append(
            remote(
                peaks_ref, peak_in.at[step], send_peak.at[step], recv_peak.at[step], "blk", target
            )
        )
    for copy in firsts + peaks:
        copy.start()
    for local in range(slot_count):
        arrived[rank * slot_count + local] = packed_ref[local, strip(rank)]

    def find(slot, places):
        live = lax.rem(slot, slot_count) < counts_ref[0, slot // slot_count]
        wanted = jnp.where(live, rows_ref[0, slot], -1)
        return tuple(
            jnp.where(wanted == row, slot, place) for row, place in enumerate(places)
        )

    places = lax.fori_loop(
        0, peers * slot_count, find, tuple(jnp.int32(0) for _ in range(row_count))
    )
    for copy in firsts:
        copy.wait_recv()
    for row in range(row_count):
        mine[row] = arrived[places[row]]

    half = row_count // 2
    quarter = half // 2

    def rank_of(order, along, across):
        x, z = (across, along) if order == 0 else (along, across)
        return (lax.rem(x + side, side) * side + lax.rem(z + side, side)) * 2 + core

    started = []

    class Route:
        def __init__(self, order):
            self.order = order
            self.at = (place_z, place_x) if order == 0 else (place_x, place_z)
            self.base = order * half
            self.counter = 0

        def source(self, hop_one, hop_two):
            return rank_of(self.order, self.at[0] + hop_one, self.at[1] + hop_two)

        def neighbour(self, axis, move):
            return self.source(move, 0) if axis == 0 else self.source(0, move)

        def rows(self, part):
            if part is None:
                return pl.ds(self.base, half)
            return pl.ds(self.base + part * quarter, quarter)

        def copy(self, slot, hop_one, hop_two, part, axis, move):
            at = self.source(hop_one, hop_two)
            rows = self.rows(part)
            if hop_one == 0 and hop_two == 0:
                source = mine.at[rows]
            else:
                source = whole_ref.at[rows, strip(at)]
            index = 20 * self.order + slot
            return remote(
                source, whole_ref.at[rows, strip(at)],
                send_two.at[index], recv_two.at[index], "blk", self.neighbour(axis, move),
            )

    near = {}

    def share_near(route, hop_one, hop_two):
        at = route.source(hop_one, hop_two)
        rows = route.rows(None)
        own = hop_one == 0 and hop_two == 0
        source = mine.at[rows] if own else whole_ref.at[rows, strip(at)]
        index = 16 * route.order + 4 * (hop_one + 1) + (hop_two + 1)
        copy = remote(
            source, whole_ref.at[rows, strip(at)],
            send_near.at[index], recv_near.at[index], "blk", partner,
        )
        copy.start()
        near[index] = copy

    routes = (Route(0), Route(1))
    sends = {}

    def launch(route, slot, hop_one, hop_two, part, axis, move):
        copy = route.copy(slot, hop_one, hop_two, part, axis, move)
        copy.start()
        sends[route.order, slot] = copy

    def arrive(route, slot):
        sends[route.order, slot].wait_recv()

    def spread(route, hop_one):
        slot = 4 + 4 * (hop_one + 1)
        launch(route, slot, hop_one, 0, None, 1, 1)
        launch(route, slot + 1, hop_one, 0, None, 1, -1)
        share_near(route, hop_one, 0)

    def along(route, move):
        arrive(route, 0 if move < 0 else 1)
        launch(route, 2 if move < 0 else 3, move, 0, 0 if move < 0 else 1, 0, -move)

    def across(route, hop_one, move):
        slot = 4 + 4 * (hop_one + 1)
        arrive(route, slot if move < 0 else slot + 1)
        launch(
            route, slot + (2 if move < 0 else 3), hop_one, move, 0 if move < 0 else 1, 1, -move
        )
        share_near(route, hop_one, move)

    for route in routes:
        launch(route, 0, 0, 0, None, 0, 1)
        launch(route, 1, 0, 0, None, 0, -1)
    for route in routes:
        spread(route, 0)
    whole_ref[:, strip(rank)] = mine[...]
    top = peaks_ref[...]
    for step, copy in enumerate(peaks, 1):
        copy.wait_recv()
        top = jnp.maximum(top, peak_in[step])
    peak_own[...] = top
    tops = []
    for step in range(1, groups):
        tops.append(
            remote(
                peak_own, peak_out.at[step], send_top.at[step], recv_top.at[step],
                "grp", lax.rem(group + step, groups),
            )
        )
    for copy in tops:
        copy.start()
    for move in (-1, 1):
        for route in routes:
            along(route, move)
        for route in routes:
            spread(route, move)
    for move in (-1, 1):
        for route in routes:
            across(route, 0, move)
    for route in routes:
        arrive(route, 2)
        arrive(route, 3)
        spread(route, 2)
    for step, copy in enumerate(tops, 1):
        copy.wait_recv()
        top = jnp.maximum(top, peak_out[step])
    off_ref[...] = top
    for hop_one in (-1, 1, 2):
        for move in (-1, 1):
            for route in routes:
                across(route, hop_one, move)
    for hop_one in (0, -1, 1, 2):
        for route in routes:
            slot = 4 + 4 * (hop_one + 1)
            arrive(route, slot + 2)
            arrive(route, slot + 3)
            share_near(route, hop_one, 2)
    for copy in near.values():
        copy.wait_recv()
    for copy in firsts + peaks + tops + list(sends.values()) + list(near.values()):
        copy.wait_send()


def exchange(packed, peaks, live_counts, slot_row, row_count, side, groups):
    slot_count, packed_rows, width = packed.shape
    chips = side * side
    peers = 2 * chips
    share = packed_rows // peers
    vmem = pl.BlockSpec(memory_space=pltpu.VMEM)
    smem = pl.BlockSpec(memory_space=pltpu.SMEM)
    dma = pltpu.SemaphoreType.DMA
    return pl.pallas_call(
        functools.partial(exchange_kernel, side, groups),
        name="exchange",
        out_shape=(
            jax.ShapeDtypeStruct((row_count, packed_rows, width), bf16),
            jax.ShapeDtypeStruct(peaks.shape, f32),
        ),
        in_specs=[vmem, vmem, smem, smem],
        out_specs=(vmem, vmem),
        scratch_shapes=[
            pltpu.VMEM((peers * slot_count, share, width), bf16),
            pltpu.VMEM((row_count, share, width), bf16),
            pltpu.VMEM((peers,) + peaks.shape, f32),
            pltpu.VMEM(peaks.shape, f32),
            pltpu.VMEM((groups,) + peaks.shape, f32),
            dma((peers,)), dma((peers,)), dma((40,)), dma((40,)), dma((32,)),
            dma((32,)), dma((peers,)), dma((peers,)), dma((groups,)), dma((groups,)),
        ],
        compiler_params=pltpu.CompilerParams(
            collective_id=0, has_side_effects=True, vmem_limit_bytes=16 * 1024 * 1024
        ),
        cost_estimate=pl.CostEstimate(
            flops=10**10, bytes_accessed=2 * row_count * packed_rows * width, transcendentals=0
        ),
    )(packed, peaks, live_counts, slot_row)


def update_kernel(whole_ref, grads_ref, updates_ref):
    width = whole_ref.shape[2]
    for row in range(whole_ref.shape[0]):
        blocks = {}
        start = 0
        for above in range(4):
            for below in range(above, 4):
                block = whole_ref[row, start : start + width]
                start += width
                blocks[above, below] = block
                if above != below:
                    blocks[below, above] = block.T
        factor = jnp.concatenate(
            [
                jnp.concatenate([blocks[above, below] for below in range(4)], axis=1)
                for above in range(4)
            ],
            axis=0,
        )
        updates_ref[0, row] = dot(grads_ref[0, row], factor).astype(bf16)


def update(whole, gradients):
    row_count, columns, size = gradients.shape[1:]
    rows = 2
    block = pl.BlockSpec((1, rows, columns, size), lambda row: (0, row, 0, 0))
    return pl.pallas_call(
        update_kernel,
        name="update",
        grid=(row_count // rows,),
        out_shape=jax.ShapeDtypeStruct(gradients.shape, bf16),
        in_specs=[pl.BlockSpec((rows,) + whole.shape[1:], lambda row: (row, 0, 0)), block],
        out_specs=block,
        compiler_params=pltpu.CompilerParams(vmem_limit_bytes=24 * 1024 * 1024),
        cost_estimate=pl.CostEstimate(
            flops=2 * row_count * size * size * columns,
            bytes_accessed=2 * row_count * size * columns,
            transcendentals=0,
        ),
    )(whole, gradients)


def per_device(peers, groups, statistics, gradients, live_counts, slot_row, sweeps):
    row_count, size = gradients.shape[1], gradients.shape[2]
    width = size // 4
    side = next(edge for edge in range(1, peers) if 2 * edge * edge == peers)
    packed, peaks = jacobi(statistics, live_counts, sweeps, 10 * width)
    whole, top = exchange(packed, peaks, live_counts, slot_row, row_count, side, groups)
    updates = update(whole, jnp.swapaxes(gradients, 2, 3))
    return (jnp.swapaxes(updates, 2, 3), top[:, 0])


def solution(mesh):
    in_specs = (
        P("grp", "blk", None, None),
        P("grp", None, None, "blk"),
        P("grp", None),
        P("grp", None),
        P("grp", "blk"),
    )
    out_specs = (P("grp", None, None, "blk"), P())
    return jax.shard_map(
        functools.partial(per_device, mesh.shape["blk"], mesh.shape["grp"]),
        mesh=mesh,
        in_specs=in_specs,
        out_specs=out_specs,
        check_vma=False,
    )
```

```python
import functools

import jax
import jax.numpy as jnp
from jax import lax
from jax.experimental import pallas as pl
from jax.experimental.pallas import tpu as pltpu
from jax.sharding import PartitionSpec as P

MAXS = 2

damping = 0.01
pairings = ((0, 1, 2, 3), (0, 2, 1, 3), (0, 3, 1, 2))
kappa_steps = (1.16, 1.74, 3.17, 6.2, 12.3, 24.5, 49.0, 98.0, 196.0)
bf16 = jnp.bfloat16
f32 = jnp.float32


def split(values):
    high = values.astype(bf16)
    return high, (values - high.astype(f32)).astype(bf16)


def left_parts(parts):
    high, low = parts
    return jnp.concatenate([high, high, low], axis=1)


def right_parts(parts):
    high, low = parts
    return jnp.concatenate([high, low, high], axis=0)


def dot(left, right):
    return jnp.dot(left, right, preferred_element_type=f32)


def dot3(left, right):
    return dot(left_parts(split(left)), right_parts(split(right)))


def eye_mask(size):
    shape = (size, size)
    return lax.broadcasted_iota(jnp.int32, shape, 0) == lax.broadcasted_iota(jnp.int32, shape, 1)


def angles_of(lower, coupling, upper, on_diagonal):
    lower_diag = jnp.sum(jnp.where(on_diagonal, lower, 0.0), axis=1, keepdims=True)
    upper_diag = jnp.sum(jnp.where(on_diagonal, upper, 0.0), axis=0, keepdims=True)
    difference = upper_diag - lower_diag
    total = lower_diag + upper_diag
    bottom = difference * difference + 4.0 * coupling * coupling + damping * (total * total)
    return coupling * difference / bottom


def jacobi_kernel(
    stats_ref, counts_ref, sweeps_ref, packed_ref, off_ref,
    mat, vec_high, vec_low, mid_high, mid_low, angle, powers, turn,
):
    slot_count, size, _ = mat.shape
    width = size // 4
    rank = lax.axis_index("blk")
    own_live = counts_ref[0, rank]
    on_diagonal = eye_mask(width)
    identity = jnp.where(on_diagonal, 1.0, 0.0).astype(f32)

    def span(member):
        return pl.ds(member * width, width)

    def turn_half(slot, half, pairing):
        members = pairing[2 * half : 2 * half + 2]
        columns = tuple(
            jnp.concatenate([ref[slot, :, span(member)] for member in members], axis=1)
            for ref in (vec_high, vec_low)
        )
        turned = split(dot(left_parts(columns), turn[slot, half]))
        for place, member in enumerate(members):
            inner = slice(place * width, (place + 1) * width)
            vec_high[slot, :, span(member)] = turned[0][:, inner]
            vec_low[slot, :, span(member)] = turned[1][:, inner]

    def one_round(slots, pairing, before):
        pairs = (pairing[:2], pairing[2:])
        chains = [(at, slot, half) for at, slot in enumerate(slots) for half in range(2)]
        waiting = [(slot, half) for slot in slots for half in range(2)] if before else []
        waiting = {
            point: waiting[point * len(waiting) // 4 : (point + 1) * len(waiting) // 4]
            for point in range(4)
        }

        def fill(point):
            for slot, half in waiting[point]:
                turn_half(slot, half, before)

        outers = []
        peak = jnp.zeros((1, width), f32)
        for at, slot, half in chains:
            first, second = pairs[half]
            angles = angles_of(
                mat[slot, span(first), span(first)],
                mat[slot, span(first), span(second)],
                mat[slot, span(second), span(second)],
                on_diagonal,
            )
            angle[2 * at + half] = angles
            outer = dot3(angles, angles.T)
            outers.append(outer)
            peak = jnp.maximum(peak, jnp.sum(jnp.abs(outer), axis=0, keepdims=True))
        fill(0)
        kappa = 1.0 + 0.26 * jnp.max(peak)
        count = jnp.int32(0)
        for bound in kappa_steps:
            count = count + (kappa > bound).astype(jnp.int32)
        scale = 2.0 / (1.0 + jnp.full((1, width), kappa))
        for at, slot, half in chains:
            error = (1.0 - scale) * identity - (0.25 * scale) * outers[2 * at + half]
            powers[2 * at + half, :, :width] = scale * (identity + error)
            powers[2 * at + half, :, width:] = dot3(error, error)
        fill(1)

        def double(step, carry):
            for at, slot, half in chains:
                both = powers[2 * at + half]
                high, low = split(both)
                product = dot(
                    left_parts((high[:, width:], low[:, width:])), right_parts((high, low))
                )
                powers[2 * at + half, :, :width] = both[:, :width] + product[:, :width]
                powers[2 * at + half, :, width:] = product[:, width:]
            return carry

        lax.fori_loop(0, count, double, 0)

        inverses = []
        for at, slot, half in chains:
            inverse = powers[2 * at + half, :, :width]
            inverses.append(
                inverse
                + dot(inverse.astype(bf16), powers[2 * at + half, :, width:].astype(bf16))
            )
        fill(2)
        rights = [
            dot3(inverses[2 * at + half], angle[2 * at + half]) for at, slot, half in chains
        ]
        fill(3)
        lows = [
            identity - 0.5 * dot3(angle[2 * at + half].T, rights[2 * at + half])
            for at, slot, half in chains
        ]
        flips = {}
        for at, slot, half in chains:
            top = split(2.0 * inverses[2 * at + half] - identity)
            right = split(rights[2 * at + half])
            flip = split(rights[2 * at + half].T)
            low = split(lows[2 * at + half])

            def square(kind, flipped):
                above, below = (-right[kind], flip[kind]) if flipped else (right[kind], -flip[kind])
                return jnp.concatenate(
                    [
                        jnp.concatenate([top[kind], above], axis=1),
                        jnp.concatenate([below, low[kind]], axis=1),
                    ],
                    axis=0,
                )

            flips[at, half] = left_parts((square(0, True), square(1, True)))
            rotation = right_parts((square(0, False), square(1, False)))
            turn[slot, half] = rotation
            for members in (pairs[0],) if half == 0 else pairs:
                rows = jnp.concatenate(
                    [
                        jnp.concatenate(
                            [mat[slot, span(member), span(column)] for column in pairs[half]],
                            axis=1,
                        )
                        for member in members
                    ],
                    axis=0,
                )
                middle = split(dot(left_parts(split(rows)), rotation))
                for down, member in enumerate(members):
                    for across, column in enumerate(pairs[half]):
                        tall = slice(down * width, (down + 1) * width)
                        wide = slice(across * width, (across + 1) * width)
                        mid_high[slot, span(member), span(column)] = middle[0][tall, wide]
                        mid_low[slot, span(member), span(column)] = middle[1][tall, wide]
        for at, slot, half in chains:
            order = pairs[0] + pairs[1] if half == 0 else pairs[1]
            rows = tuple(
                jnp.concatenate(
                    [
                        jnp.concatenate(
                            [ref[slot, span(member), span(column)] for column in order], axis=1
                        )
                        for member in pairs[half]
                    ],
                    axis=0,
                )
                for ref in (mid_high, mid_low)
            )
            fresh = dot(flips[at, half], right_parts(rows))
            for down, member in enumerate(pairs[half]):
                for across, column in enumerate(order):
                    block = fresh[
                        down * width : (down + 1) * width, across * width : (across + 1) * width
                    ]
                    mat[slot, span(member), span(column)] = block
                    if across > 1:
                        mat[slot, span(column), span(member)] = block.T

    def measure(sweep, slot):
        outside = jnp.zeros((1, width), f32)
        inside = jnp.zeros((1, width), f32)
        for row in range(4):
            for column in range(4):
                squares = mat[slot, span(row), span(column)]
                squares = squares * squares
                if row == column:
                    own = jnp.where(on_diagonal, squares, 0.0)
                    inside += jnp.sum(own, axis=0, keepdims=True)
                    squares = jnp.where(on_diagonal, 0.0, squares)
                outside += jnp.sum(squares, axis=0, keepdims=True)
        off_total = jnp.sum(outside, axis=1, keepdims=True)
        total = off_total + jnp.sum(inside, axis=1, keepdims=True)
        norm = jnp.broadcast_to(jnp.sqrt(off_total / total), (1, width))
        row = pl.ds(sweep, 1)
        off_ref[row, :] = jnp.maximum(off_ref[row, :], norm)

    off_ref[...] = jnp.zeros_like(off_ref)
    ident_rows = jnp.where(eye_mask(size), 1.0, 0.0).astype(bf16)

    for slot in range(slot_count):

        @pl.when(slot < own_live)
        def _():
            mat[slot] = stats_ref[0, slot]
            vec_high[slot] = ident_rows
            vec_low[slot] = jnp.zeros((size, size), bf16)

    def one_sweep(sweep, carry):
        active = [
            jnp.logical_and(slot < own_live, sweeps_ref[0, slot] > sweep)
            for slot in range(slot_count)
        ]

        def run(slots):
            for before, pairing in zip((None,) + pairings, pairings):
                one_round(slots, pairing, before)
            for slot in slots:
                for half in range(2):
                    turn_half(slot, half, pairings[-1])
            for slot in slots:
                measure(sweep, slot)

        for slot in range(0, slot_count, 2):
            if slot + 1 == slot_count:
                pl.when(active[slot])(functools.partial(run, (slot,)))
                continue
            pl.when(jnp.logical_and(active[slot], active[slot + 1]))(
                functools.partial(run, (slot, slot + 1))
            )
            single = jnp.where(active[slot], slot, slot + 1)
            pl.when(jnp.logical_xor(active[slot], active[slot + 1]))(
                functools.partial(run, (single,))
            )
        return carry

    lax.fori_loop(0, MAXS, one_sweep, 0)

    for slot in range(slot_count):

        @pl.when(slot < own_live)
        def _():
            diagonal = jnp.concatenate(
                [
                    jnp.sum(
                        jnp.where(on_diagonal, mat[slot, span(member), span(member)], 0.0),
                        axis=0,
                        keepdims=True,
                    )
                    for member in range(4)
                ],
                axis=1,
            )
            scales = lax.rsqrt(jnp.sqrt(jnp.sqrt(diagonal)))
            vectors = vec_high[slot].astype(f32) + vec_low[slot].astype(f32)
            high, low = split(vectors * scales)
            mid_high[slot] = high
            mid_low[slot] = low
            for tile in range(2):
                tall, wide = 2 * width * (tile + 1), pl.ds(2 * width * tile, 2 * width)
                left = jnp.concatenate(
                    [mid_high[slot, :tall], mid_high[slot, :tall], mid_low[slot, :tall]], axis=1
                )
                right = jnp.concatenate(
                    [mid_high[slot, wide], mid_low[slot, wide], mid_high[slot, wide]], axis=1
                )
                strip = lax.dot_general(
                    left, right, (((1,), (1,)), ((), ())), preferred_element_type=f32
                ).astype(bf16)
                for column in (2 * tile, 2 * tile + 1):
                    for row in range(column + 1):
                        start = (4 * row - row * (row - 1) // 2 + column - row) * width
                        packed_ref[slot, start : start + width] = strip[
                            row * width : (row + 1) * width,
                            (column - 2 * tile) * width : (column - 2 * tile + 1) * width,
                        ]


def jacobi(statistics, live_counts, sweeps, packed_rows):
    slot_count, size = statistics.shape[1], statistics.shape[2]
    width = size // 4
    vmem = pl.BlockSpec(memory_space=pltpu.VMEM)
    smem = pl.BlockSpec(memory_space=pltpu.SMEM)
    return pl.pallas_call(
        jacobi_kernel,
        name="jacobi",
        out_shape=(
            jax.ShapeDtypeStruct((slot_count, packed_rows, width), bf16),
            jax.ShapeDtypeStruct((MAXS, width), f32),
        ),
        in_specs=[vmem, smem, smem],
        out_specs=(vmem, vmem),
        scratch_shapes=[
            pltpu.VMEM((slot_count, size, size), f32),
            pltpu.VMEM((slot_count, size, size), bf16),
            pltpu.VMEM((slot_count, size, size), bf16),
            pltpu.VMEM((slot_count, size, size), bf16),
            pltpu.VMEM((slot_count, size, size), bf16),
            pltpu.VMEM((4, width, width), f32),
            pltpu.VMEM((4, width, 2 * width), f32),
            pltpu.VMEM((slot_count, 2, 6 * width, 2 * width), bf16),
        ],
        compiler_params=pltpu.CompilerParams(vmem_limit_bytes=24 * 1024 * 1024),
        cost_estimate=pl.CostEstimate(
            flops=10**10, bytes_accessed=4 * slot_count * size * size, transcendentals=0
        ),
    )(statistics, live_counts, sweeps)


def exchange_kernel(
    side, groups, packed_ref, peaks_ref, counts_ref, rows_ref, whole_ref, off_ref,
    arrived, mine, peak_in, peak_own, peak_out,
    send_one, recv_one, send_two, recv_two, send_near, recv_near, send_peak, recv_peak, send_top, recv_top,
):
    chips = side * side
    peers = 2 * chips
    rank = lax.axis_index("blk")
    group = lax.axis_index("grp")
    slot_count = packed_ref.shape[0]
    row_count, share = mine.shape[0], mine.shape[1]
    core = lax.rem(rank, 2)
    place_x, place_z = rank // (2 * side), lax.rem(rank // 2, side)
    partner = rank + 1 - 2 * core

    def remote(source, target, send_sem, recv_sem, axis, index):
        return pltpu.make_async_remote_copy(
            src_ref=source,
            dst_ref=target,
            send_sem=send_sem,
            recv_sem=recv_sem,
            device_id={axis: index},
            device_id_type=pl.DeviceIdType.MESH,
        )

    barrier = pltpu.get_barrier_semaphore()
    for step in range(1, peers):
        pl.semaphore_signal(
            barrier, inc=1, device_id={"blk": lax.rem(rank + step, peers)},
            device_id_type=pl.DeviceIdType.MESH,
        )
    for step in range(1, groups):
        pl.semaphore_signal(
            barrier, inc=1, device_id={"grp": lax.rem(group + step, groups)},
            device_id_type=pl.DeviceIdType.MESH,
        )
    pl.semaphore_wait(barrier, peers + groups - 2)

    def strip(index):
        return pl.ds(pl.multiple_of(index * share, share), share)

    firsts, peaks = [], []
    own_slots = pl.ds(rank * slot_count, slot_count)
    for step in range(1, peers):
        target = lax.rem(rank + step, peers)
        firsts.append(
            remote(
                packed_ref.at[:, strip(target)],
                arrived.at[own_slots], send_one.at[step], recv_one.at[step], "blk", target,
            )
        )
        peaks.append(
            remote(
                peaks_ref, peak_in.at[step], send_peak.at[step], recv_peak.at[step], "blk", target
            )
        )
    for copy in firsts + peaks:
        copy.start()
    for local in range(slot_count):
        arrived[rank * slot_count + local] = packed_ref[local, strip(rank)]

    def find(slot, places):
        live = lax.rem(slot, slot_count) < counts_ref[0, slot // slot_count]
        wanted = jnp.where(live, rows_ref[0, slot], -1)
        return tuple(
            jnp.where(wanted == row, slot, place) for row, place in enumerate(places)
        )

    places = lax.fori_loop(
        0, peers * slot_count, find, tuple(jnp.int32(0) for _ in range(row_count))
    )
    for copy in firsts:
        copy.wait_recv()
    for row in range(row_count):
        mine[row] = arrived[places[row]]

    half = row_count // 2
    quarter = half // 2

    def rank_of(order, along, across):
        x, z = (across, along) if order == 0 else (along, across)
        return (lax.rem(x + side, side) * side + lax.rem(z + side, side)) * 2 + core

    started = []

    class Route:
        def __init__(self, order):
            self.order = order
            self.at = (place_z, place_x) if order == 0 else (place_x, place_z)
            self.base = order * half
            self.counter = 0

        def source(self, hop_one, hop_two):
            return rank_of(self.order, self.at[0] + hop_one, self.at[1] + hop_two)

        def neighbour(self, axis, move):
            return self.source(move, 0) if axis == 0 else self.source(0, move)

        def rows(self, part):
            if part is None:
                return pl.ds(self.base, half)
            return pl.ds(self.base + part * quarter, quarter)

        def copy(self, slot, hop_one, hop_two, part, axis, move):
            at = self.source(hop_one, hop_two)
            rows = self.rows(part)
            if hop_one == 0 and hop_two == 0:
                source = mine.at[rows]
            else:
                source = whole_ref.at[rows, strip(at)]
            index = 20 * self.order + slot
            return remote(
                source, whole_ref.at[rows, strip(at)],
                send_two.at[index], recv_two.at[index], "blk", self.neighbour(axis, move),
            )

    near = {}

    def share_near(route, hop_one, hop_two):
        at = route.source(hop_one, hop_two)
        rows = route.rows(None)
        own = hop_one == 0 and hop_two == 0
        source = mine.at[rows] if own else whole_ref.at[rows, strip(at)]
        index = 16 * route.order + 4 * (hop_one + 1) + (hop_two + 1)
        copy = remote(
            source, whole_ref.at[rows, strip(at)],
            send_near.at[index], recv_near.at[index], "blk", partner,
        )
        copy.start()
        near[index] = copy

    routes = (Route(0), Route(1))
    sends = {}

    def launch(route, slot, hop_one, hop_two, part, axis, move):
        copy = route.copy(slot, hop_one, hop_two, part, axis, move)
        copy.start()
        sends[route.order, slot] = copy

    def arrive(route, slot):
        sends[route.order, slot].wait_recv()

    def spread(route, hop_one):
        slot = 4 + 4 * (hop_one + 1)
        launch(route, slot, hop_one, 0, None, 1, 1)
        launch(route, slot + 1, hop_one, 0, None, 1, -1)
        share_near(route, hop_one, 0)

    def along(route, move):
        arrive(route, 0 if move < 0 else 1)
        launch(route, 2 if move < 0 else 3, move, 0, 0 if move < 0 else 1, 0, -move)

    def across(route, hop_one, move):
        slot = 4 + 4 * (hop_one + 1)
        arrive(route, slot if move < 0 else slot + 1)
        launch(
            route, slot + (2 if move < 0 else 3), hop_one, move, 0 if move < 0 else 1, 1, -move
        )
        share_near(route, hop_one, move)

    for route in routes:
        launch(route, 0, 0, 0, None, 0, 1)
        launch(route, 1, 0, 0, None, 0, -1)
    for route in routes:
        spread(route, 0)
    whole_ref[:, strip(rank)] = mine[...]
    top = peaks_ref[...]
    for step, copy in enumerate(peaks, 1):
        copy.wait_recv()
        top = jnp.maximum(top, peak_in[step])
    peak_own[...] = top
    tops = []
    for step in range(1, groups):
        tops.append(
            remote(
                peak_own, peak_out.at[step], send_top.at[step], recv_top.at[step],
                "grp", lax.rem(group + step, groups),
            )
        )
    for copy in tops:
        copy.start()
    for move in (-1, 1):
        for route in routes:
            along(route, move)
        for route in routes:
            spread(route, move)
    for move in (-1, 1):
        for route in routes:
            across(route, 0, move)
    for route in routes:
        arrive(route, 2)
        arrive(route, 3)
        spread(route, 2)
    for step, copy in enumerate(tops, 1):
        copy.wait_recv()
        top = jnp.maximum(top, peak_out[step])
    off_ref[...] = top
    for hop_one in (-1, 1, 2):
        for move in (-1, 1):
            for route in routes:
                across(route, hop_one, move)
    for hop_one in (0, -1, 1, 2):
        for route in routes:
            slot = 4 + 4 * (hop_one + 1)
            arrive(route, slot + 2)
            arrive(route, slot + 3)
            share_near(route, hop_one, 2)
    for copy in near.values():
        copy.wait_recv()
    for copy in firsts + peaks + tops + list(sends.values()) + list(near.values()):
        copy.wait_send()


def exchange(packed, peaks, live_counts, slot_row, row_count, side, groups):
    slot_count, packed_rows, width = packed.shape
    chips = side * side
    peers = 2 * chips
    share = packed_rows // peers
    vmem = pl.BlockSpec(memory_space=pltpu.VMEM)
    smem = pl.BlockSpec(memory_space=pltpu.SMEM)
    dma = pltpu.SemaphoreType.DMA
    return pl.pallas_call(
        functools.partial(exchange_kernel, side, groups),
        name="exchange",
        out_shape=(
            jax.ShapeDtypeStruct((row_count, packed_rows, width), bf16),
            jax.ShapeDtypeStruct(peaks.shape, f32),
        ),
        in_specs=[vmem, vmem, smem, smem],
        out_specs=(vmem, vmem),
        scratch_shapes=[
            pltpu.VMEM((peers * slot_count, share, width), bf16),
            pltpu.VMEM((row_count, share, width), bf16),
            pltpu.VMEM((peers,) + peaks.shape, f32),
            pltpu.VMEM(peaks.shape, f32),
            pltpu.VMEM((groups,) + peaks.shape, f32),
            dma((peers,)), dma((peers,)), dma((40,)), dma((40,)), dma((32,)),
            dma((32,)), dma((peers,)), dma((peers,)), dma((groups,)), dma((groups,)),
        ],
        compiler_params=pltpu.CompilerParams(
            collective_id=0, has_side_effects=True, vmem_limit_bytes=16 * 1024 * 1024
        ),
        cost_estimate=pl.CostEstimate(
            flops=10**10, bytes_accessed=2 * row_count * packed_rows * width, transcendentals=0
        ),
    )(packed, peaks, live_counts, slot_row)


def update_kernel(whole_ref, grads_ref, peaks_ref, updates_ref, off_ref):
    @pl.when(pl.program_id(0) == 0)
    def _():
        for sweep in range(MAXS):
            off_ref[sweep] = jnp.max(peaks_ref[sweep : sweep + 1])

    width = whole_ref.shape[2]
    for row in range(whole_ref.shape[0]):
        blocks = {}
        start = 0
        for above in range(4):
            for below in range(above, 4):
                block = whole_ref[row, start : start + width]
                start += width
                blocks[above, below] = block
                if above != below:
                    blocks[below, above] = block.T
        factor = jnp.concatenate(
            [
                jnp.concatenate([blocks[above, below] for below in range(4)], axis=1)
                for above in range(4)
            ],
            axis=0,
        )
        updates_ref[0, row] = dot(grads_ref[0, row], factor).astype(bf16)


def update(whole, gradients, peaks):
    row_count, columns, size = gradients.shape[1:]
    rows = 4
    block = pl.BlockSpec((1, rows, columns, size), lambda row: (0, row, 0, 0))
    return pl.pallas_call(
        update_kernel,
        name="update",
        grid=(row_count // rows,),
        out_shape=(
            jax.ShapeDtypeStruct(gradients.shape, bf16),
            jax.ShapeDtypeStruct((MAXS,), f32),
        ),
        in_specs=[
            pl.BlockSpec((rows,) + whole.shape[1:], lambda row: (row, 0, 0)),
            block,
            pl.BlockSpec(memory_space=pltpu.VMEM),
        ],
        out_specs=(block, pl.BlockSpec(memory_space=pltpu.SMEM)),
        compiler_params=pltpu.CompilerParams(vmem_limit_bytes=24 * 1024 * 1024),
        cost_estimate=pl.CostEstimate(
            flops=2 * row_count * size * size * columns,
            bytes_accessed=2 * row_count * size * columns,
            transcendentals=0,
        ),
    )(whole, gradients, peaks)


def per_device(peers, groups, statistics, gradients, live_counts, slot_row, sweeps):
    row_count, size = gradients.shape[1], gradients.shape[2]
    width = size // 4
    side = next(edge for edge in range(1, peers) if 2 * edge * edge == peers)
    packed, peaks = jacobi(statistics, live_counts, sweeps, 10 * width)
    whole, top = exchange(packed, peaks, live_counts, slot_row, row_count, side, groups)
    updates, off = update(whole, jnp.swapaxes(gradients, 2, 3), top)
    return (jnp.swapaxes(updates, 2, 3), off)


def solution(mesh):
    in_specs = (
        P("grp", "blk", None, None),
        P("grp", None, None, "blk"),
        P("grp", None),
        P("grp", None),
        P("grp", "blk"),
    )
    out_specs = (P("grp", None, None, "blk"), P())
    return jax.shard_map(
        functools.partial(per_device, mesh.shape["blk"], mesh.shape["grp"]),
        mesh=mesh,
        in_specs=in_specs,
        out_specs=out_specs,
        check_vma=False,
    )
```

```python
import functools

import jax
import jax.numpy as jnp
from jax import lax
from jax.experimental import pallas as pl
from jax.experimental.pallas import tpu as pltpu
from jax.sharding import PartitionSpec as P

MAXS = 2

damping = 0.01
apart = ((0, 1), (0, 2), (0, 3), (1, 2), (1, 3), (2, 3))
pairings = ((0, 1, 2, 3), (0, 2, 1, 3), (0, 3, 1, 2))
kappa_steps = (1.16, 1.74, 3.17, 6.2, 12.3, 24.5, 49.0, 98.0, 196.0)
bf16 = jnp.bfloat16
f32 = jnp.float32


def split(values):
    high = values.astype(bf16)
    return high, (values - high.astype(f32)).astype(bf16)


def left_parts(parts):
    high, low = parts
    return jnp.concatenate([high, high, low], axis=1)


def right_parts(parts):
    high, low = parts
    return jnp.concatenate([high, low, high], axis=0)


def dot(left, right):
    return jnp.dot(left, right, preferred_element_type=f32)


def dot3(left, right):
    return dot(left_parts(split(left)), right_parts(split(right)))


def eye_mask(size):
    shape = (size, size)
    return lax.broadcasted_iota(jnp.int32, shape, 0) == lax.broadcasted_iota(jnp.int32, shape, 1)


def upper_mask(size):
    shape = (size, size)
    return lax.broadcasted_iota(jnp.int32, shape, 0) <= lax.broadcasted_iota(jnp.int32, shape, 1)


def angles_of(lower, coupling, upper, on_diagonal):
    lower_diag = jnp.sum(jnp.where(on_diagonal, lower, 0.0), axis=1, keepdims=True)
    upper_diag = jnp.sum(jnp.where(on_diagonal, upper, 0.0), axis=0, keepdims=True)
    difference = upper_diag - lower_diag
    total = lower_diag + upper_diag
    bottom = difference * difference + 4.0 * coupling * coupling + damping * (total * total)
    return coupling * difference / bottom


def jacobi_kernel(
    stats_ref, counts_ref, sweeps_ref, packed_ref, off_ref,
    mat, vec_high, vec_low, mid_high, mid_low, angle, powers, turn,
):
    slot_count, size, _ = mat.shape
    width = size // 4
    rank = lax.axis_index("blk")
    own_live = counts_ref[0, rank]
    on_diagonal = eye_mask(width)
    upper = upper_mask(width)
    identity = jnp.where(on_diagonal, 1.0, 0.0).astype(f32)

    def span(member):
        return pl.ds(member * width, width)

    def turn_half(slot, half, pairing):
        members = pairing[2 * half : 2 * half + 2]
        columns = tuple(
            jnp.concatenate([ref[slot, :, span(member)] for member in members], axis=1)
            for ref in (vec_high, vec_low)
        )
        turned = split(dot(left_parts(columns), turn[slot, half]))
        for place, member in enumerate(members):
            inner = slice(place * width, (place + 1) * width)
            vec_high[slot, :, span(member)] = turned[0][:, inner]
            vec_low[slot, :, span(member)] = turned[1][:, inner]

    def one_round(slots, pairing, before):
        pairs = (pairing[:2], pairing[2:])
        chains = [(at, slot, half) for at, slot in enumerate(slots) for half in range(2)]
        waiting = [(slot, half) for slot in slots for half in range(2)] if before else []
        waiting = {
            point: waiting[point * len(waiting) // 4 : (point + 1) * len(waiting) // 4]
            for point in range(4)
        }

        def fill(point):
            for slot, half in waiting[point]:
                turn_half(slot, half, before)

        outers = []
        peak = jnp.zeros((1, width), f32)
        for at, slot, half in chains:
            first, second = pairs[half]
            angles = angles_of(
                mat[slot, span(first), span(first)],
                mat[slot, span(first), span(second)],
                mat[slot, span(second), span(second)],
                on_diagonal,
            )
            angle[2 * at + half] = angles
            outer = dot3(angles, angles.T)
            outers.append(outer)
            peak = jnp.maximum(peak, jnp.sum(jnp.abs(outer), axis=0, keepdims=True))
        fill(0)
        kappa = 1.0 + 0.26 * jnp.max(peak)
        count = jnp.int32(0)
        for bound in kappa_steps:
            count = count + (kappa > bound).astype(jnp.int32)
        scale = 2.0 / (1.0 + jnp.full((1, width), kappa))
        for at, slot, half in chains:
            error = (1.0 - scale) * identity - (0.25 * scale) * outers[2 * at + half]
            powers[2 * at + half, :, :width] = scale * (identity + error)
            powers[2 * at + half, :, width:] = dot3(error, error)
        fill(1)

        def double(step, carry):
            for at, slot, half in chains:
                both = powers[2 * at + half]
                high, low = split(both)
                product = dot(
                    left_parts((high[:, width:], low[:, width:])), right_parts((high, low))
                )
                powers[2 * at + half, :, :width] = both[:, :width] + product[:, :width]
                powers[2 * at + half, :, width:] = product[:, width:]
            return carry

        lax.fori_loop(0, count, double, 0)

        inverses = []
        for at, slot, half in chains:
            inverse = powers[2 * at + half, :, :width]
            inverses.append(
                inverse
                + dot(inverse.astype(bf16), powers[2 * at + half, :, width:].astype(bf16))
            )
        fill(2)
        rights = [
            dot3(inverses[2 * at + half], angle[2 * at + half]) for at, slot, half in chains
        ]
        fill(3)
        lows = [
            identity - 0.5 * dot3(angle[2 * at + half].T, rights[2 * at + half])
            for at, slot, half in chains
        ]
        flips = {}
        for at, slot, half in chains:
            top = split(2.0 * inverses[2 * at + half] - identity)
            right = split(rights[2 * at + half])
            flip = split(rights[2 * at + half].T)
            low = split(lows[2 * at + half])

            def square(kind, flipped):
                above, below = (-right[kind], flip[kind]) if flipped else (right[kind], -flip[kind])
                return jnp.concatenate(
                    [
                        jnp.concatenate([top[kind], above], axis=1),
                        jnp.concatenate([below, low[kind]], axis=1),
                    ],
                    axis=0,
                )

            flips[at, half] = left_parts((square(0, True), square(1, True)))
            rotation = right_parts((square(0, False), square(1, False)))
            turn[slot, half] = rotation
            for members in (pairs[0],) if half == 0 else pairs:
                rows = jnp.concatenate(
                    [
                        jnp.concatenate(
                            [mat[slot, span(member), span(column)] for column in pairs[half]],
                            axis=1,
                        )
                        for member in members
                    ],
                    axis=0,
                )
                middle = split(dot(left_parts(split(rows)), rotation))
                for down, member in enumerate(members):
                    for across, column in enumerate(pairs[half]):
                        tall = slice(down * width, (down + 1) * width)
                        wide = slice(across * width, (across + 1) * width)
                        mid_high[slot, span(member), span(column)] = middle[0][tall, wide]
                        mid_low[slot, span(member), span(column)] = middle[1][tall, wide]
        for at, slot, half in chains:
            order = pairs[0] + pairs[1] if half == 0 else pairs[1]
            rows = tuple(
                jnp.concatenate(
                    [
                        jnp.concatenate(
                            [ref[slot, span(member), span(column)] for column in order], axis=1
                        )
                        for member in pairs[half]
                    ],
                    axis=0,
                )
                for ref in (mid_high, mid_low)
            )
            fresh = dot(flips[at, half], right_parts(rows))
            for down, member in enumerate(pairs[half]):
                for across, column in enumerate(order):
                    block = fresh[
                        down * width : (down + 1) * width, across * width : (across + 1) * width
                    ]
                    mat[slot, span(member), span(column)] = block
                    if across > 1:
                        mat[slot, span(column), span(member)] = block.T

    def measure(sweep, slot):
        outside = jnp.zeros((1, width), f32)
        inside = jnp.zeros((1, width), f32)
        for row in range(4):
            for column in range(4):
                squares = mat[slot, span(row), span(column)]
                squares = squares * squares
                if row == column:
                    own = jnp.where(on_diagonal, squares, 0.0)
                    inside += jnp.sum(own, axis=0, keepdims=True)
                    squares = jnp.where(on_diagonal, 0.0, squares)
                outside += jnp.sum(squares, axis=0, keepdims=True)
        off_total = jnp.sum(outside, axis=1, keepdims=True)
        total = off_total + jnp.sum(inside, axis=1, keepdims=True)
        norm = jnp.broadcast_to(jnp.sqrt(off_total / total), (1, width))
        row = pl.ds(sweep, 1)
        off_ref[0, row, :] = jnp.maximum(off_ref[0, row, :], norm)

    off_ref[0] = jnp.zeros(off_ref.shape[1:], f32)
    ident_rows = jnp.where(eye_mask(size), 1.0, 0.0).astype(bf16)

    for slot in range(slot_count):

        @pl.when(slot < own_live)
        def _():
            mat[slot] = stats_ref[0, slot]
            vec_high[slot] = ident_rows
            vec_low[slot] = jnp.zeros((size, size), bf16)

    def one_sweep(sweep, carry):
        active = [
            jnp.logical_and(slot < own_live, sweeps_ref[0, slot] > sweep)
            for slot in range(slot_count)
        ]

        def run(slots):
            for before, pairing in zip((None,) + pairings, pairings):
                one_round(slots, pairing, before)
            for slot in slots:
                for half in range(2):
                    turn_half(slot, half, pairings[-1])
            for slot in slots:
                measure(sweep, slot)

        for slot in range(0, slot_count, 2):
            if slot + 1 == slot_count:
                pl.when(active[slot])(functools.partial(run, (slot,)))
                continue
            pl.when(jnp.logical_and(active[slot], active[slot + 1]))(
                functools.partial(run, (slot, slot + 1))
            )
            single = jnp.where(active[slot], slot, slot + 1)
            pl.when(jnp.logical_xor(active[slot], active[slot + 1]))(
                functools.partial(run, (single,))
            )
        return carry

    lax.fori_loop(0, MAXS, one_sweep, 0)

    for slot in range(slot_count):

        @pl.when(slot < own_live)
        def _():
            diagonal = jnp.concatenate(
                [
                    jnp.sum(
                        jnp.where(on_diagonal, mat[slot, span(member), span(member)], 0.0),
                        axis=0,
                        keepdims=True,
                    )
                    for member in range(4)
                ],
                axis=1,
            )
            scales = lax.rsqrt(jnp.sqrt(jnp.sqrt(diagonal)))
            vectors = vec_high[slot].astype(f32) + vec_low[slot].astype(f32)
            high, low = split(vectors * scales)
            mid_high[slot] = high
            mid_low[slot] = low
            for tile in range(2):
                tall, wide = 2 * width * (tile + 1), pl.ds(2 * width * tile, 2 * width)
                left = jnp.concatenate(
                    [mid_high[slot, :tall], mid_high[slot, :tall], mid_low[slot, :tall]], axis=1
                )
                right = jnp.concatenate(
                    [mid_high[slot, wide], mid_low[slot, wide], mid_high[slot, wide]], axis=1
                )
                strip = lax.dot_general(
                    left, right, (((1,), (1,)), ((), ())), preferred_element_type=f32
                )

                def block(row, column):
                    across = column - 2 * tile
                    return strip[
                        row * width : (row + 1) * width, across * width : (across + 1) * width
                    ]

                first, second = block(2 * tile, 2 * tile), block(2 * tile + 1, 2 * tile + 1)
                packed_ref[slot, tile * width : (tile + 1) * width] = jnp.where(
                    upper, first, second
                ).astype(bf16)
                off_ref[1 + slot, tile : tile + 1] = jnp.sum(
                    jnp.where(on_diagonal, second.astype(bf16).astype(f32), 0.0),
                    axis=0,
                    keepdims=True,
                )
                for start, (row, column) in enumerate(apart, 2):
                    if column // 2 == tile:
                        packed_ref[slot, start * width : (start + 1) * width] = block(
                            row, column
                        ).astype(bf16)


def jacobi(statistics, live_counts, sweeps, packed_rows):
    slot_count, size = statistics.shape[1], statistics.shape[2]
    width = size // 4
    vmem = pl.BlockSpec(memory_space=pltpu.VMEM)
    smem = pl.BlockSpec(memory_space=pltpu.SMEM)
    return pl.pallas_call(
        jacobi_kernel,
        name="jacobi",
        out_shape=(
            jax.ShapeDtypeStruct((slot_count, packed_rows, width), bf16),
            jax.ShapeDtypeStruct((1 + slot_count, 2, width), f32),
        ),
        in_specs=[vmem, smem, smem],
        out_specs=(vmem, vmem),
        scratch_shapes=[
            pltpu.VMEM((slot_count, size, size), f32),
            pltpu.VMEM((slot_count, size, size), bf16),
            pltpu.VMEM((slot_count, size, size), bf16),
            pltpu.VMEM((slot_count, size, size), bf16),
            pltpu.VMEM((slot_count, size, size), bf16),
            pltpu.VMEM((4, width, width), f32),
            pltpu.VMEM((4, width, 2 * width), f32),
            pltpu.VMEM((slot_count, 2, 6 * width, 2 * width), bf16),
        ],
        compiler_params=pltpu.CompilerParams(vmem_limit_bytes=24 * 1024 * 1024),
        cost_estimate=pl.CostEstimate(
            flops=10**10, bytes_accessed=4 * slot_count * size * size, transcendentals=0
        ),
    )(statistics, live_counts, sweeps)


def exchange_kernel(
    side, groups, packed_ref, peaks_ref, counts_ref, rows_ref, whole_ref, edges_ref, off_ref,
    arrived, mine, peak_in, peak_own, peak_out,
    send_one, recv_one, send_two, recv_two, send_near, recv_near, send_peak, recv_peak, send_top, recv_top,
):
    chips = side * side
    peers = 2 * chips
    rank = lax.axis_index("blk")
    group = lax.axis_index("grp")
    slot_count = packed_ref.shape[0]
    row_count, share = mine.shape[0], mine.shape[1]
    core = lax.rem(rank, 2)
    place_x, place_z = rank // (2 * side), lax.rem(rank // 2, side)
    partner = rank + 1 - 2 * core

    def remote(source, target, send_sem, recv_sem, axis, index):
        return pltpu.make_async_remote_copy(
            src_ref=source,
            dst_ref=target,
            send_sem=send_sem,
            recv_sem=recv_sem,
            device_id={axis: index},
            device_id_type=pl.DeviceIdType.MESH,
        )

    barrier = pltpu.get_barrier_semaphore()
    for step in range(1, peers):
        pl.semaphore_signal(
            barrier, inc=1, device_id={"blk": lax.rem(rank + step, peers)},
            device_id_type=pl.DeviceIdType.MESH,
        )
    for step in range(1, groups):
        pl.semaphore_signal(
            barrier, inc=1, device_id={"grp": lax.rem(group + step, groups)},
            device_id_type=pl.DeviceIdType.MESH,
        )
    pl.semaphore_wait(barrier, peers + groups - 2)

    def strip(index):
        return pl.ds(pl.multiple_of(index * share, share), share)

    firsts, peaks = [], []
    own_slots = pl.ds(rank * slot_count, slot_count)
    for step in range(1, peers):
        target = lax.rem(rank + step, peers)
        firsts.append(
            remote(
                packed_ref.at[:, strip(target)],
                arrived.at[own_slots], send_one.at[step], recv_one.at[step], "blk", target,
            )
        )
        peaks.append(
            remote(
                peaks_ref, peak_in.at[rank], send_peak.at[step], recv_peak.at[step], "blk", target
            )
        )
    for copy in firsts + peaks:
        copy.start()
    peak_in[rank] = peaks_ref[...]
    for local in range(slot_count):
        arrived[rank * slot_count + local] = packed_ref[local, strip(rank)]

    def find(slot, places):
        live = lax.rem(slot, slot_count) < counts_ref[0, slot // slot_count]
        wanted = jnp.where(live, rows_ref[0, slot], -1)
        return tuple(
            jnp.where(wanted == row, slot, place) for row, place in enumerate(places)
        )

    places = lax.fori_loop(
        0, peers * slot_count, find, tuple(jnp.int32(0) for _ in range(row_count))
    )
    for copy in firsts:
        copy.wait_recv()
    for row in range(row_count):
        mine[row] = arrived[places[row]]

    half = row_count // 2
    quarter = half // 2

    def rank_of(order, along, across):
        x, z = (across, along) if order == 0 else (along, across)
        return (lax.rem(x + side, side) * side + lax.rem(z + side, side)) * 2 + core

    started = []

    class Route:
        def __init__(self, order):
            self.order = order
            self.at = (place_z, place_x) if order == 0 else (place_x, place_z)
            self.base = order * half
            self.counter = 0

        def source(self, hop_one, hop_two):
            return rank_of(self.order, self.at[0] + hop_one, self.at[1] + hop_two)

        def neighbour(self, axis, move):
            return self.source(move, 0) if axis == 0 else self.source(0, move)

        def rows(self, part):
            if part is None:
                return pl.ds(self.base, half)
            return pl.ds(self.base + part * quarter, quarter)

        def copy(self, slot, hop_one, hop_two, part, axis, move):
            at = self.source(hop_one, hop_two)
            rows = self.rows(part)
            if hop_one == 0 and hop_two == 0:
                source = mine.at[rows]
            else:
                source = whole_ref.at[rows, strip(at)]
            index = 20 * self.order + slot
            return remote(
                source, whole_ref.at[rows, strip(at)],
                send_two.at[index], recv_two.at[index], "blk", self.neighbour(axis, move),
            )

    near = {}

    def share_near(route, hop_one, hop_two):
        at = route.source(hop_one, hop_two)
        rows = route.rows(None)
        own = hop_one == 0 and hop_two == 0
        source = mine.at[rows] if own else whole_ref.at[rows, strip(at)]
        index = 16 * route.order + 4 * (hop_one + 1) + (hop_two + 1)
        copy = remote(
            source, whole_ref.at[rows, strip(at)],
            send_near.at[index], recv_near.at[index], "blk", partner,
        )
        copy.start()
        near[index] = copy

    routes = (Route(0), Route(1))
    sends = {}

    def launch(route, slot, hop_one, hop_two, part, axis, move):
        copy = route.copy(slot, hop_one, hop_two, part, axis, move)
        copy.start()
        sends[route.order, slot] = copy

    def arrive(route, slot):
        sends[route.order, slot].wait_recv()

    def spread(route, hop_one):
        slot = 4 + 4 * (hop_one + 1)
        launch(route, slot, hop_one, 0, None, 1, 1)
        launch(route, slot + 1, hop_one, 0, None, 1, -1)
        share_near(route, hop_one, 0)

    def along(route, move):
        arrive(route, 0 if move < 0 else 1)
        launch(route, 2 if move < 0 else 3, move, 0, 0 if move < 0 else 1, 0, -move)

    def across(route, hop_one, move):
        slot = 4 + 4 * (hop_one + 1)
        arrive(route, slot if move < 0 else slot + 1)
        launch(
            route, slot + (2 if move < 0 else 3), hop_one, move, 0 if move < 0 else 1, 1, -move
        )
        share_near(route, hop_one, move)

    for route in routes:
        launch(route, 0, 0, 0, None, 0, 1)
        launch(route, 1, 0, 0, None, 0, -1)
    for route in routes:
        spread(route, 0)
    whole_ref[:, strip(rank)] = mine[...]
    for copy in peaks:
        copy.wait_recv()
    top = peak_in[0, 0]
    for owner in range(1, peers):
        top = jnp.maximum(top, peak_in[owner, 0])
    for row in range(row_count):
        edges_ref[row] = peak_in[places[row] // slot_count, 1 + lax.rem(places[row], slot_count)]
    peak_own[...] = top
    tops = []
    for step in range(1, groups):
        tops.append(
            remote(
                peak_own, peak_out.at[step], send_top.at[step], recv_top.at[step],
                "grp", lax.rem(group + step, groups),
            )
        )
    for copy in tops:
        copy.start()
    for move in (-1, 1):
        for route in routes:
            along(route, move)
        for route in routes:
            spread(route, move)
    for move in (-1, 1):
        for route in routes:
            across(route, 0, move)
    for route in routes:
        arrive(route, 2)
        arrive(route, 3)
        spread(route, 2)
    for step, copy in enumerate(tops, 1):
        copy.wait_recv()
        top = jnp.maximum(top, peak_out[step])
    off_ref[...] = top
    for hop_one in (-1, 1, 2):
        for move in (-1, 1):
            for route in routes:
                across(route, hop_one, move)
    for hop_one in (0, -1, 1, 2):
        for route in routes:
            slot = 4 + 4 * (hop_one + 1)
            arrive(route, slot + 2)
            arrive(route, slot + 3)
            share_near(route, hop_one, 2)
    for copy in near.values():
        copy.wait_recv()
    for copy in firsts + peaks + tops + list(sends.values()) + list(near.values()):
        copy.wait_send()


def exchange(packed, peaks, live_counts, slot_row, row_count, side, groups):
    slot_count, packed_rows, width = packed.shape
    chips = side * side
    peers = 2 * chips
    share = packed_rows // peers
    vmem = pl.BlockSpec(memory_space=pltpu.VMEM)
    smem = pl.BlockSpec(memory_space=pltpu.SMEM)
    dma = pltpu.SemaphoreType.DMA
    return pl.pallas_call(
        functools.partial(exchange_kernel, side, groups),
        name="exchange",
        out_shape=(
            jax.ShapeDtypeStruct((row_count, packed_rows, width), bf16),
            jax.ShapeDtypeStruct((row_count,) + peaks.shape[1:], f32),
            jax.ShapeDtypeStruct(peaks.shape[1:], f32),
        ),
        in_specs=[vmem, vmem, smem, smem],
        out_specs=(vmem, vmem, vmem),
        scratch_shapes=[
            pltpu.VMEM((peers * slot_count, share, width), bf16),
            pltpu.VMEM((row_count, share, width), bf16),
            pltpu.VMEM((peers,) + peaks.shape, f32),
            pltpu.VMEM(peaks.shape[1:], f32),
            pltpu.VMEM((groups,) + peaks.shape[1:], f32),
            dma((peers,)), dma((peers,)), dma((40,)), dma((40,)), dma((32,)),
            dma((32,)), dma((peers,)), dma((peers,)), dma((groups,)), dma((groups,)),
        ],
        compiler_params=pltpu.CompilerParams(
            collective_id=0, has_side_effects=True, vmem_limit_bytes=16 * 1024 * 1024
        ),
        cost_estimate=pl.CostEstimate(
            flops=10**10, bytes_accessed=2 * row_count * packed_rows * width, transcendentals=0
        ),
    )(packed, peaks, live_counts, slot_row)


def update_kernel(whole_ref, edges_ref, grads_ref, peaks_ref, updates_ref, off_ref):
    @pl.when(pl.program_id(0) == 0)
    def _():
        for sweep in range(MAXS):
            off_ref[sweep] = jnp.max(peaks_ref[sweep : sweep + 1])

    width = whole_ref.shape[2]
    upper, on_diagonal = upper_mask(width), eye_mask(width)
    for row in range(whole_ref.shape[0]):
        blocks = {}
        for start, where in enumerate(apart, 2):
            blocks[where] = whole_ref[row, start * width : (start + 1) * width]
        for side, above in enumerate((0, 2)):
            both = whole_ref[row, side * width : (side + 1) * width]
            flipped = both.T
            edge = jnp.where(on_diagonal, edges_ref[row, side : side + 1], 0.0).astype(bf16)
            blocks[above, above] = jnp.where(upper, both, flipped)
            blocks[above + 1, above + 1] = jnp.where(
                on_diagonal, edge, jnp.where(upper, flipped, both)
            )
            blocks[above + 1, above] = blocks[above, above + 1].T

        def tile(first, second):
            return jnp.concatenate(
                [
                    jnp.concatenate([blocks[above, below] for below in (second, second + 1)], axis=1)
                    for above in (first, first + 1)
                ],
                axis=0,
            )

        corner = tile(0, 2)
        left, right = grads_ref[0, row, :, : 2 * width], grads_ref[0, row, :, 2 * width :]
        turned = lax.dot_general(
            right, corner, (((1,), (1,)), ((), ())), preferred_element_type=f32
        )
        updates_ref[0, row, :, : 2 * width] = (dot(left, tile(0, 0)) + turned).astype(bf16)
        updates_ref[0, row, :, 2 * width :] = (dot(left, corner) + dot(right, tile(2, 2))).astype(
            bf16
        )


def update(whole, edges, gradients, peaks):
    row_count, columns, size = gradients.shape[1:]
    rows = 4
    block = pl.BlockSpec((1, rows, columns, size), lambda row: (0, row, 0, 0))
    return pl.pallas_call(
        update_kernel,
        name="update",
        grid=(row_count // rows,),
        out_shape=(
            jax.ShapeDtypeStruct(gradients.shape, bf16),
            jax.ShapeDtypeStruct((MAXS,), f32),
        ),
        in_specs=[
            pl.BlockSpec((rows,) + whole.shape[1:], lambda row: (row, 0, 0)),
            pl.BlockSpec((rows,) + edges.shape[1:], lambda row: (row, 0, 0)),
            block,
            pl.BlockSpec(memory_space=pltpu.VMEM),
        ],
        out_specs=(block, pl.BlockSpec(memory_space=pltpu.SMEM)),
        compiler_params=pltpu.CompilerParams(vmem_limit_bytes=24 * 1024 * 1024),
        cost_estimate=pl.CostEstimate(
            flops=2 * row_count * size * size * columns,
            bytes_accessed=2 * row_count * size * columns,
            transcendentals=0,
        ),
    )(whole, edges, gradients, peaks)


def per_device(peers, groups, statistics, gradients, live_counts, slot_row, sweeps):
    row_count, size = gradients.shape[1], gradients.shape[2]
    width = size // 4
    side = next(edge for edge in range(1, peers) if 2 * edge * edge == peers)
    packed, peaks = jacobi(statistics, live_counts, sweeps, 8 * width)
    whole, edges, top = exchange(packed, peaks, live_counts, slot_row, row_count, side, groups)
    updates, off = update(whole, edges, jnp.swapaxes(gradients, 2, 3), top)
    return (jnp.swapaxes(updates, 2, 3), off)


def solution(mesh):
    in_specs = (
        P("grp", "blk", None, None),
        P("grp", None, None, "blk"),
        P("grp", None),
        P("grp", None),
        P("grp", "blk"),
    )
    out_specs = (P("grp", None, None, "blk"), P())
    return jax.shard_map(
        functools.partial(per_device, mesh.shape["blk"], mesh.shape["grp"]),
        mesh=mesh,
        in_specs=in_specs,
        out_specs=out_specs,
        check_vma=False,
    )
```

```python
import functools

import jax
import jax.numpy as jnp
from jax import lax
from jax.experimental import pallas as pl
from jax.experimental.pallas import tpu as pltpu
from jax.sharding import PartitionSpec as P

MAXS = 2

damping = 0.01
apart = ((0, 1), (0, 2), (0, 3), (1, 2), (1, 3), (2, 3))
pairings = ((0, 1, 2, 3), (0, 2, 1, 3), (0, 3, 1, 2))
kappa_steps = (1.16, 1.74, 3.17, 6.2, 12.3, 24.5, 49.0, 98.0, 196.0)
bf16 = jnp.bfloat16
f32 = jnp.float32


def split(values):
    high = values.astype(bf16)
    return high, (values - high.astype(f32)).astype(bf16)


def left_parts(parts):
    high, low = parts
    return jnp.concatenate([high, high, low], axis=1)


def right_parts(parts):
    high, low = parts
    return jnp.concatenate([high, low, high], axis=0)


def dot(left, right):
    return jnp.dot(left, right, preferred_element_type=f32)


def dot3(left, right):
    return dot(left_parts(split(left)), right_parts(split(right)))


def eye_mask(size):
    shape = (size, size)
    return lax.broadcasted_iota(jnp.int32, shape, 0) == lax.broadcasted_iota(jnp.int32, shape, 1)


def upper_mask(size):
    shape = (size, size)
    return lax.broadcasted_iota(jnp.int32, shape, 0) <= lax.broadcasted_iota(jnp.int32, shape, 1)


def angles_of(lower, coupling, upper, on_diagonal):
    lower_diag = jnp.sum(jnp.where(on_diagonal, lower, 0.0), axis=1, keepdims=True)
    upper_diag = jnp.sum(jnp.where(on_diagonal, upper, 0.0), axis=0, keepdims=True)
    difference = upper_diag - lower_diag
    total = lower_diag + upper_diag
    bottom = difference * difference + 4.0 * coupling * coupling + damping * (total * total)
    return coupling * difference / bottom


def jacobi_kernel(
    stats_ref, counts_ref, sweeps_ref, packed_ref, off_ref,
    mat, vec_high, vec_low, mid_high, mid_low, angle, powers, turn,
):
    slot_count, size, _ = mat.shape
    width = size // 4
    rank = lax.axis_index("blk")
    own_live = counts_ref[0, rank]
    on_diagonal = eye_mask(width)
    upper = upper_mask(width)
    identity = jnp.where(on_diagonal, 1.0, 0.0).astype(f32)

    def span(member):
        return pl.ds(member * width, width)

    def turn_half(slot, half, pairing):
        members = pairing[2 * half : 2 * half + 2]
        columns = tuple(
            jnp.concatenate([ref[slot, :, span(member)] for member in members], axis=1)
            for ref in (vec_high, vec_low)
        )
        turned = split(dot(left_parts(columns), turn[slot, half]))
        for place, member in enumerate(members):
            inner = slice(place * width, (place + 1) * width)
            vec_high[slot, :, span(member)] = turned[0][:, inner]
            vec_low[slot, :, span(member)] = turned[1][:, inner]

    def one_round(slots, pairing, before):
        pairs = (pairing[:2], pairing[2:])
        chains = [(at, slot, half) for at, slot in enumerate(slots) for half in range(2)]
        waiting = [(slot, half) for slot in slots for half in range(2)] if before else []
        waiting = {
            point: waiting[point * len(waiting) // 4 : (point + 1) * len(waiting) // 4]
            for point in range(4)
        }

        def fill(point):
            for slot, half in waiting[point]:
                turn_half(slot, half, before)

        outers = []
        peak = jnp.zeros((1, width), f32)
        for at, slot, half in chains:
            first, second = pairs[half]
            angles = angles_of(
                mat[slot, span(first), span(first)],
                mat[slot, span(first), span(second)],
                mat[slot, span(second), span(second)],
                on_diagonal,
            )
            angle[2 * at + half] = angles
            outer = dot3(angles, angles.T)
            outers.append(outer)
            peak = jnp.maximum(peak, jnp.sum(jnp.abs(outer), axis=0, keepdims=True))
        fill(0)
        kappa = 1.0 + 0.26 * jnp.max(peak)
        count = jnp.int32(0)
        for bound in kappa_steps:
            count = count + (kappa > bound).astype(jnp.int32)
        scale = 2.0 / (1.0 + jnp.full((1, width), kappa))
        for at, slot, half in chains:
            error = (1.0 - scale) * identity - (0.25 * scale) * outers[2 * at + half]
            powers[2 * at + half, :, :width] = scale * (identity + error)
            powers[2 * at + half, :, width:] = dot3(error, error)
        fill(1)

        def double(step, carry):
            for at, slot, half in chains:
                both = powers[2 * at + half]
                high, low = split(both)
                product = dot(
                    left_parts((high[:, width:], low[:, width:])), right_parts((high, low))
                )
                powers[2 * at + half, :, :width] = both[:, :width] + product[:, :width]
                powers[2 * at + half, :, width:] = product[:, width:]
            return carry

        lax.fori_loop(0, count, double, 0)

        inverses = []
        for at, slot, half in chains:
            inverse = powers[2 * at + half, :, :width]
            inverses.append(
                inverse
                + dot(inverse.astype(bf16), powers[2 * at + half, :, width:].astype(bf16))
            )
        fill(2)
        rights = [
            dot3(inverses[2 * at + half], angle[2 * at + half]) for at, slot, half in chains
        ]
        fill(3)
        lows = [
            identity - 0.5 * dot3(angle[2 * at + half].T, rights[2 * at + half])
            for at, slot, half in chains
        ]
        flips = {}
        for at, slot, half in chains:
            top = split(2.0 * inverses[2 * at + half] - identity)
            right = split(rights[2 * at + half])
            flip = split(rights[2 * at + half].T)
            low = split(lows[2 * at + half])

            def square(kind, flipped):
                above, below = (-right[kind], flip[kind]) if flipped else (right[kind], -flip[kind])
                return jnp.concatenate(
                    [
                        jnp.concatenate([top[kind], above], axis=1),
                        jnp.concatenate([below, low[kind]], axis=1),
                    ],
                    axis=0,
                )

            flips[at, half] = left_parts((square(0, True), square(1, True)))
            rotation = right_parts((square(0, False), square(1, False)))
            turn[slot, half] = rotation
            for members in (pairs[0],) if half == 0 else pairs:
                rows = jnp.concatenate(
                    [
                        jnp.concatenate(
                            [mat[slot, span(member), span(column)] for column in pairs[half]],
                            axis=1,
                        )
                        for member in members
                    ],
                    axis=0,
                )
                middle = split(dot(left_parts(split(rows)), rotation))
                for down, member in enumerate(members):
                    for across, column in enumerate(pairs[half]):
                        tall = slice(down * width, (down + 1) * width)
                        wide = slice(across * width, (across + 1) * width)
                        mid_high[slot, span(member), span(column)] = middle[0][tall, wide]
                        mid_low[slot, span(member), span(column)] = middle[1][tall, wide]
        for at, slot, half in chains:
            order = pairs[0] + pairs[1] if half == 0 else pairs[1]
            rows = tuple(
                jnp.concatenate(
                    [
                        jnp.concatenate(
                            [ref[slot, span(member), span(column)] for column in order], axis=1
                        )
                        for member in pairs[half]
                    ],
                    axis=0,
                )
                for ref in (mid_high, mid_low)
            )
            fresh = dot(flips[at, half], right_parts(rows))
            for down, member in enumerate(pairs[half]):
                for across, column in enumerate(order):
                    block = fresh[
                        down * width : (down + 1) * width, across * width : (across + 1) * width
                    ]
                    mat[slot, span(member), span(column)] = block
                    if across > 1:
                        mat[slot, span(column), span(member)] = block.T

    def measure(sweep, slot):
        outside = jnp.zeros((1, width), f32)
        inside = jnp.zeros((1, width), f32)
        for row in range(4):
            for column in range(4):
                squares = mat[slot, span(row), span(column)]
                squares = squares * squares
                if row == column:
                    own = jnp.where(on_diagonal, squares, 0.0)
                    inside += jnp.sum(own, axis=0, keepdims=True)
                    squares = jnp.where(on_diagonal, 0.0, squares)
                outside += jnp.sum(squares, axis=0, keepdims=True)
        off_total = jnp.sum(outside, axis=1, keepdims=True)
        total = off_total + jnp.sum(inside, axis=1, keepdims=True)
        norm = jnp.broadcast_to(jnp.sqrt(off_total / total), (1, width))
        row = pl.ds(sweep, 1)
        off_ref[0, row, :] = jnp.maximum(off_ref[0, row, :], norm)

    off_ref[0] = jnp.zeros(off_ref.shape[1:], f32)
    ident_rows = jnp.where(eye_mask(size), 1.0, 0.0).astype(bf16)

    for slot in range(slot_count):

        @pl.when(slot < own_live)
        def _():
            mat[slot] = stats_ref[0, slot]
            vec_high[slot] = ident_rows
            vec_low[slot] = jnp.zeros((size, size), bf16)

    def one_sweep(sweep, carry):
        active = [
            jnp.logical_and(slot < own_live, sweeps_ref[0, slot] > sweep)
            for slot in range(slot_count)
        ]

        def run(slots):
            for before, pairing in zip((None,) + pairings, pairings):
                one_round(slots, pairing, before)
            for slot in slots:
                for half in range(2):
                    turn_half(slot, half, pairings[-1])
            for slot in slots:
                measure(sweep, slot)

        for slot in range(0, slot_count, 2):
            if slot + 1 == slot_count:
                pl.when(active[slot])(functools.partial(run, (slot,)))
                continue
            pl.when(jnp.logical_and(active[slot], active[slot + 1]))(
                functools.partial(run, (slot, slot + 1))
            )
            single = jnp.where(active[slot], slot, slot + 1)
            pl.when(jnp.logical_xor(active[slot], active[slot + 1]))(
                functools.partial(run, (single,))
            )
        return carry

    lax.fori_loop(0, MAXS, one_sweep, 0)

    for slot in range(slot_count):

        @pl.when(slot < own_live)
        def _():
            diagonal = jnp.concatenate(
                [
                    jnp.sum(
                        jnp.where(on_diagonal, mat[slot, span(member), span(member)], 0.0),
                        axis=0,
                        keepdims=True,
                    )
                    for member in range(4)
                ],
                axis=1,
            )
            scales = lax.rsqrt(jnp.sqrt(jnp.sqrt(diagonal)))
            vectors = vec_high[slot].astype(f32) + vec_low[slot].astype(f32)
            high, low = split(vectors * scales)
            mid_high[slot] = high
            mid_low[slot] = low
            for tile in range(2):
                tall, wide = 2 * width * (tile + 1), pl.ds(2 * width * tile, 2 * width)
                left = jnp.concatenate(
                    [mid_high[slot, :tall], mid_high[slot, :tall], mid_low[slot, :tall]], axis=1
                )
                right = jnp.concatenate(
                    [mid_high[slot, wide], mid_low[slot, wide], mid_high[slot, wide]], axis=1
                )
                strip = lax.dot_general(
                    left, right, (((1,), (1,)), ((), ())), preferred_element_type=f32
                )

                def block(row, column):
                    across = column - 2 * tile
                    return strip[
                        row * width : (row + 1) * width, across * width : (across + 1) * width
                    ]

                first, second = block(2 * tile, 2 * tile), block(2 * tile + 1, 2 * tile + 1)
                packed_ref[slot, tile * width : (tile + 1) * width] = jnp.where(
                    upper, first, second
                ).astype(bf16)
                off_ref[1 + slot, tile : tile + 1] = jnp.sum(
                    jnp.where(on_diagonal, second.astype(bf16).astype(f32), 0.0),
                    axis=0,
                    keepdims=True,
                )
                for start, (row, column) in enumerate(apart, 2):
                    if column // 2 == tile:
                        packed_ref[slot, start * width : (start + 1) * width] = block(
                            row, column
                        ).astype(bf16)


def jacobi(statistics, live_counts, sweeps, packed_rows):
    slot_count, size = statistics.shape[1], statistics.shape[2]
    width = size // 4
    vmem = pl.BlockSpec(memory_space=pltpu.VMEM)
    smem = pl.BlockSpec(memory_space=pltpu.SMEM)
    return pl.pallas_call(
        jacobi_kernel,
        name="jacobi",
        out_shape=(
            jax.ShapeDtypeStruct((slot_count, packed_rows, width), bf16),
            jax.ShapeDtypeStruct((1 + slot_count, 2, width), f32),
        ),
        in_specs=[vmem, smem, smem],
        out_specs=(vmem, vmem),
        scratch_shapes=[
            pltpu.VMEM((slot_count, size, size), f32),
            pltpu.VMEM((slot_count, size, size), bf16),
            pltpu.VMEM((slot_count, size, size), bf16),
            pltpu.VMEM((slot_count, size, size), bf16),
            pltpu.VMEM((slot_count, size, size), bf16),
            pltpu.VMEM((4, width, width), f32),
            pltpu.VMEM((4, width, 2 * width), f32),
            pltpu.VMEM((slot_count, 2, 6 * width, 2 * width), bf16),
        ],
        compiler_params=pltpu.CompilerParams(vmem_limit_bytes=24 * 1024 * 1024),
        cost_estimate=pl.CostEstimate(
            flops=10**10, bytes_accessed=4 * slot_count * size * size, transcendentals=0
        ),
    )(statistics, live_counts, sweeps)


def exchange_kernel(
    side, groups, packed_ref, peaks_ref, counts_ref, rows_ref, whole_ref, edges_ref, off_ref,
    arrived, mine, peak_in, peak_own, peak_out,
    send_one, recv_one, send_two, recv_two, send_near, recv_near, send_peak, recv_peak, send_top, recv_top,
):
    chips = side * side
    peers = 2 * chips
    rank = lax.axis_index("blk")
    group = lax.axis_index("grp")
    slot_count = packed_ref.shape[0]
    row_count, share = mine.shape[0], mine.shape[1]
    core = lax.rem(rank, 2)
    place_x, place_z = rank // (2 * side), lax.rem(rank // 2, side)
    partner = rank + 1 - 2 * core

    def remote(source, target, send_sem, recv_sem, axis, index):
        return pltpu.make_async_remote_copy(
            src_ref=source,
            dst_ref=target,
            send_sem=send_sem,
            recv_sem=recv_sem,
            device_id={axis: index},
            device_id_type=pl.DeviceIdType.MESH,
        )

    barrier = pltpu.get_barrier_semaphore()
    ring = [(lead, lag) for lead in range(side) for lag in range(side)]
    offsets = [(lead, lag, flip) for lead, lag in ring for flip in range(2)]

    def hops(offset):
        lead, lag, flip = offset
        return -(min(lead, side - lead) + min(lag, side - lag)), -flip

    targets = [
        (
            lax.rem(place_x + lead, side) * side + lax.rem(place_z + lag, side)
        ) * 2 + (1 - core if flip else core)
        for lead, lag, flip in sorted(offsets, key=hops)[:-1]
    ]
    for target in targets:
        pl.semaphore_signal(
            barrier, inc=1, device_id={"blk": target},
            device_id_type=pl.DeviceIdType.MESH,
        )
    for step in range(1, groups):
        pl.semaphore_signal(
            barrier, inc=1, device_id={"grp": lax.rem(group + step, groups)},
            device_id_type=pl.DeviceIdType.MESH,
        )
    pl.semaphore_wait(barrier, peers + groups - 2)

    def strip(index):
        return pl.ds(pl.multiple_of(index * share, share), share)

    firsts, peaks = [], []
    own_slots = pl.ds(rank * slot_count, slot_count)
    for step, target in enumerate(targets):
        firsts.append(
            remote(
                packed_ref.at[:, strip(target)],
                arrived.at[own_slots], send_one.at[step], recv_one.at[step], "blk", target,
            )
        )
        peaks.append(
            remote(
                peaks_ref, peak_in.at[rank], send_peak.at[step], recv_peak.at[step], "blk", target
            )
        )
    for copy in firsts + peaks:
        copy.start()
    peak_in[rank] = peaks_ref[...]
    for local in range(slot_count):
        arrived[rank * slot_count + local] = packed_ref[local, strip(rank)]

    def find(slot, places):
        live = lax.rem(slot, slot_count) < counts_ref[0, slot // slot_count]
        wanted = jnp.where(live, rows_ref[0, slot], -1)
        return tuple(
            jnp.where(wanted == row, slot, place) for row, place in enumerate(places)
        )

    places = lax.fori_loop(
        0, peers * slot_count, find, tuple(jnp.int32(0) for _ in range(row_count))
    )
    for copy in firsts:
        copy.wait_recv()
    for row in range(row_count):
        mine[row] = arrived[places[row]]

    half = row_count // 2
    quarter = half // 2

    def rank_of(order, along, across):
        x, z = (across, along) if order == 0 else (along, across)
        return (lax.rem(x + side, side) * side + lax.rem(z + side, side)) * 2 + core

    started = []

    class Route:
        def __init__(self, order):
            self.order = order
            self.at = (place_z, place_x) if order == 0 else (place_x, place_z)
            self.base = order * half
            self.counter = 0

        def source(self, hop_one, hop_two):
            return rank_of(self.order, self.at[0] + hop_one, self.at[1] + hop_two)

        def neighbour(self, axis, move):
            return self.source(move, 0) if axis == 0 else self.source(0, move)

        def rows(self, part):
            if part is None:
                return pl.ds(self.base, half)
            return pl.ds(self.base + part * quarter, quarter)

        def copy(self, slot, hop_one, hop_two, part, axis, move):
            at = self.source(hop_one, hop_two)
            rows = self.rows(part)
            if hop_one == 0 and hop_two == 0:
                source = mine.at[rows]
            else:
                source = whole_ref.at[rows, strip(at)]
            index = 20 * self.order + slot
            return remote(
                source, whole_ref.at[rows, strip(at)],
                send_two.at[index], recv_two.at[index], "blk", self.neighbour(axis, move),
            )

    near = {}

    def share_near(route, hop_one, hop_two):
        at = route.source(hop_one, hop_two)
        rows = route.rows(None)
        own = hop_one == 0 and hop_two == 0
        source = mine.at[rows] if own else whole_ref.at[rows, strip(at)]
        index = 16 * route.order + 4 * (hop_one + 1) + (hop_two + 1)
        copy = remote(
            source, whole_ref.at[rows, strip(at)],
            send_near.at[index], recv_near.at[index], "blk", partner,
        )
        copy.start()
        near[index] = copy

    routes = (Route(0), Route(1))
    sends = {}

    def launch(route, slot, hop_one, hop_two, part, axis, move):
        copy = route.copy(slot, hop_one, hop_two, part, axis, move)
        copy.start()
        sends[route.order, slot] = copy

    def arrive(route, slot):
        sends[route.order, slot].wait_recv()

    def spread(route, hop_one):
        slot = 4 + 4 * (hop_one + 1)
        launch(route, slot, hop_one, 0, None, 1, 1)
        launch(route, slot + 1, hop_one, 0, None, 1, -1)
        share_near(route, hop_one, 0)

    def along(route, move):
        arrive(route, 0 if move < 0 else 1)
        launch(route, 2 if move < 0 else 3, move, 0, 0 if move < 0 else 1, 0, -move)

    def across(route, hop_one, move):
        slot = 4 + 4 * (hop_one + 1)
        arrive(route, slot if move < 0 else slot + 1)
        launch(
            route, slot + (2 if move < 0 else 3), hop_one, move, 0 if move < 0 else 1, 1, -move
        )
        share_near(route, hop_one, move)

    for route in routes:
        launch(route, 0, 0, 0, None, 0, 1)
        launch(route, 1, 0, 0, None, 0, -1)
    for route in routes:
        spread(route, 0)
    whole_ref[:, strip(rank)] = mine[...]
    for copy in peaks:
        copy.wait_recv()
    top = peak_in[0, 0]
    for owner in range(1, peers):
        top = jnp.maximum(top, peak_in[owner, 0])
    for row in range(row_count):
        edges_ref[row] = peak_in[places[row] // slot_count, 1 + lax.rem(places[row], slot_count)]
    peak_own[...] = top
    tops = []
    for step in range(1, groups):
        tops.append(
            remote(
                peak_own, peak_out.at[step], send_top.at[step], recv_top.at[step],
                "grp", lax.rem(group + step, groups),
            )
        )
    for copy in tops:
        copy.start()
    for move in (-1, 1):
        for route in routes:
            along(route, move)
        for route in routes:
            spread(route, move)
    for move in (-1, 1):
        for route in routes:
            across(route, 0, move)
    for route in routes:
        arrive(route, 2)
        arrive(route, 3)
        spread(route, 2)
    for step, copy in enumerate(tops, 1):
        copy.wait_recv()
        top = jnp.maximum(top, peak_out[step])
    off_ref[...] = top
    for hop_one in (-1, 1, 2):
        for move in (-1, 1):
            for route in routes:
                across(route, hop_one, move)
    for hop_one in (0, -1, 1, 2):
        for route in routes:
            slot = 4 + 4 * (hop_one + 1)
            arrive(route, slot + 2)
            arrive(route, slot + 3)
            share_near(route, hop_one, 2)
    for copy in near.values():
        copy.wait_recv()
    for copy in firsts + peaks + tops + list(sends.values()) + list(near.values()):
        copy.wait_send()


def exchange(packed, peaks, live_counts, slot_row, row_count, side, groups):
    slot_count, packed_rows, width = packed.shape
    chips = side * side
    peers = 2 * chips
    share = packed_rows // peers
    vmem = pl.BlockSpec(memory_space=pltpu.VMEM)
    smem = pl.BlockSpec(memory_space=pltpu.SMEM)
    dma = pltpu.SemaphoreType.DMA
    return pl.pallas_call(
        functools.partial(exchange_kernel, side, groups),
        name="exchange",
        out_shape=(
            jax.ShapeDtypeStruct((row_count, packed_rows, width), bf16),
            jax.ShapeDtypeStruct((row_count,) + peaks.shape[1:], f32),
            jax.ShapeDtypeStruct(peaks.shape[1:], f32),
        ),
        in_specs=[vmem, vmem, smem, smem],
        out_specs=(vmem, vmem, vmem),
        scratch_shapes=[
            pltpu.VMEM((peers * slot_count, share, width), bf16),
            pltpu.VMEM((row_count, share, width), bf16),
            pltpu.VMEM((peers,) + peaks.shape, f32),
            pltpu.VMEM(peaks.shape[1:], f32),
            pltpu.VMEM((groups,) + peaks.shape[1:], f32),
            dma((peers,)), dma((peers,)), dma((40,)), dma((40,)), dma((32,)),
            dma((32,)), dma((peers,)), dma((peers,)), dma((groups,)), dma((groups,)),
        ],
        compiler_params=pltpu.CompilerParams(
            collective_id=0, has_side_effects=True, vmem_limit_bytes=16 * 1024 * 1024
        ),
        cost_estimate=pl.CostEstimate(
            flops=10**10, bytes_accessed=2 * row_count * packed_rows * width, transcendentals=0
        ),
    )(packed, peaks, live_counts, slot_row)


def update_kernel(
    whole_ref, edges_ref, grads_ref, peaks_ref, updates_ref, off_ref, done, sent
):
    width = whole_ref.shape[2]
    row_count = whole_ref.shape[0]
    upper, on_diagonal = upper_mask(width), eye_mask(width)
    for sweep in range(MAXS):
        off_ref[sweep] = jnp.max(peaks_ref[sweep : sweep + 1])

    def leave(row):
        return pltpu.make_async_copy(done.at[row], updates_ref.at[0, row], sent.at[row])

    def one_row(row):
        blocks = {}
        for start, where in enumerate(apart, 2):
            blocks[where] = whole_ref[row, start * width : (start + 1) * width]
        for side, above in enumerate((0, 2)):
            both = whole_ref[row, side * width : (side + 1) * width]
            flipped = both.T
            edge = jnp.where(on_diagonal, edges_ref[row, side : side + 1], 0.0).astype(bf16)
            blocks[above, above] = jnp.where(upper, both, flipped)
            blocks[above + 1, above + 1] = jnp.where(
                on_diagonal, edge, jnp.where(upper, flipped, both)
            )
            blocks[above + 1, above] = blocks[above, above + 1].T

        def tile(first, second):
            return jnp.concatenate(
                [
                    jnp.concatenate([blocks[above, below] for below in (second, second + 1)], axis=1)
                    for above in (first, first + 1)
                ],
                axis=0,
            )

        corner = tile(0, 2)
        left, right = grads_ref[0, row, :, : 2 * width], grads_ref[0, row, :, 2 * width :]
        turned = lax.dot_general(
            right, corner, (((1,), (1,)), ((), ())), preferred_element_type=f32
        )
        done[row, :, : 2 * width] = (dot(left, tile(0, 0)) + turned).astype(bf16)
        done[row, :, 2 * width :] = (dot(left, corner) + dot(right, tile(2, 2))).astype(
            bf16
        )

    for row in range(row_count):
        one_row(row)
        if row:
            leave(row - 1).start()
    leave(row_count - 1).start()
    for row in range(row_count):
        leave(row).wait()


def update(whole, edges, gradients, peaks):
    row_count, columns, size = gradients.shape[1:]
    vmem = pl.BlockSpec(memory_space=pltpu.VMEM)
    return pl.pallas_call(
        update_kernel,
        name="update",
        out_shape=(
            jax.ShapeDtypeStruct(gradients.shape, bf16),
            jax.ShapeDtypeStruct((MAXS,), f32),
        ),
        in_specs=[vmem] * 4,
        out_specs=(pl.BlockSpec(memory_space=pl.ANY), pl.BlockSpec(memory_space=pltpu.SMEM)),
        scratch_shapes=[
            pltpu.VMEM(gradients.shape[1:], bf16),
            pltpu.SemaphoreType.DMA((row_count,)),
        ],
        compiler_params=pltpu.CompilerParams(vmem_limit_bytes=24 * 1024 * 1024),
        cost_estimate=pl.CostEstimate(
            flops=2 * row_count * size * size * columns,
            bytes_accessed=2 * row_count * size * columns,
            transcendentals=0,
        ),
    )(whole, edges, gradients, peaks)


def per_device(peers, groups, statistics, gradients, live_counts, slot_row, sweeps):
    row_count, size = gradients.shape[1], gradients.shape[2]
    width = size // 4
    side = next(edge for edge in range(1, peers) if 2 * edge * edge == peers)
    packed, peaks = jacobi(statistics, live_counts, sweeps, 8 * width)
    whole, edges, top = exchange(packed, peaks, live_counts, slot_row, row_count, side, groups)
    updates, off = update(whole, edges, jnp.swapaxes(gradients, 2, 3), top)
    return (jnp.swapaxes(updates, 2, 3), off)


def solution(mesh):
    in_specs = (
        P("grp", "blk", None, None),
        P("grp", None, None, "blk"),
        P("grp", None),
        P("grp", None),
        P("grp", "blk"),
    )
    out_specs = (P("grp", None, None, "blk"), P())
    return jax.shard_map(
        functools.partial(per_device, mesh.shape["blk"], mesh.shape["grp"]),
        mesh=mesh,
        in_specs=in_specs,
        out_specs=out_specs,
        check_vma=False,
    )
```
